512 devices in a mesh: seq: 64 (over z_lo, y, core), head: 8 (over x, z_hi).
Axes of the slice: x: 4, y: 8, z: 8 (z_hi: 2, z_lo: 4; z = z_hi * 4 + z_lo), core: 2. Of those that a mesh axis runs over, the one named last changes fastest.
Arguments:
- att_q: bfloat16 [16384, 5120], P('seq', 'head'), may hold values from -150 to 150
- att_k: bfloat16 [16384, 5120], P('seq', 'head'), may hold values from -6 to 6
- att_v: bfloat16 [16384, 5120], P('seq', 'head'), may hold values from -6 to 6
- fast_q: bfloat16 [16384, 5120], P('seq', 'head'), may hold values from -6 to 6
- fast_k: bfloat16 [16384, 5120], P('seq', 'head'), may hold values from -6 to 6
- fast_v: bfloat16 [16384, 5120], P('seq', 'head'), may hold values from -6 to 6
- learn_rates: float32 [16384], P('seq'), may hold values from 0.0002 to 0.002
- w_gate: bfloat16 [640, 5120], P(None, 'head'), may hold values from -0.25 to 0.25
- w_up: bfloat16 [640, 5120], P(None, 'head'), may hold values from -0.25 to 0.25
- w_down: bfloat16 [640, 5120], P(None, 'head'), may hold values from -0.25 to 0.25
Outputs:
- attended: bfloat16 [16384, 5120], P('seq', 'head')
- fast_out: bfloat16 [16384, 5120], P('seq', 'head')
The draws below stay inside these ranges and needn't reach their ends.
All inputs are finite; a program needn't handle non-finite values.
Results may differ from the reference program's by a relative error of at most 0.007.
The reference program's roundings to bfloat16 on the way (of `softmax_w` and `hidden_q`) count: a program that leaves them out, or rounds other values in their place, can miss the bound.
Values may be sent and summed in bfloat16 or wider, within the bound.
A program may use at most 64 MiB of HBM per device.

```python
import math
import jax
import jax.numpy as jnp
from jax import lax

TOK_DEV = 256
WINDOW = 1024
HEAD_DIM = 128
FAST_D = 640
FAST_HID = 640
TOKENS = 16384
AHEADS = 40
FHEADS = 8


def attention_pair(key):
    base_key = jax.random.fold_in(key, 31)
    arr_shape = (TOKENS, AHEADS * HEAD_DIM)
    query_all = jnp.clip(jax.random.normal(jax.random.fold_in(base_key, 1), arr_shape, jnp.float32), -5.0, 5.0)
    keys_all = jnp.clip(jax.random.normal(jax.random.fold_in(base_key, 2), arr_shape, jnp.float32), -5.0, 5.0)
    return (query_all, keys_all)


def draw_att_q(key, part):
    return attention_pair(key)[0].astype(jnp.bfloat16)


def draw_att_k(key, part):
    return attention_pair(key)[1].astype(jnp.bfloat16)


def shard_levels(key, extent, pieces, low, top_value):
    factor_of, own = 1.0, jax.random.fold_in(key, 6)
    for axis_at, blocks in pieces:
        draws = jnp.exp(jax.random.uniform(jax.random.fold_in(own, axis_at), (blocks,), jnp.float32, low / len(pieces), top_value / len(pieces)))
        factor_of = factor_of * jnp.repeat(draws, extent[axis_at] // blocks).reshape([-1 if axis == axis_at else 1 for axis in range(len(extent))])
    return factor_of


def centred(stream_key, dims, scale, limit, split=(), kind=jnp.bfloat16):
    values = jax.random.normal(stream_key, dims, jnp.float32) * scale
    if len(split) > 0:
        values = shard_levels(stream_key, dims, split, -0.22, 0.18) * values
    return jnp.clip(values, min=-limit, max=limit).astype(kind)


def setup_inputs(seed: int = 0) -> dict:
    splits = jax.random.split(jax.random.key(seed), 11)
    att_q = draw_att_q(jax.random.fold_in(splits[10], 71), 0)
    att_k = draw_att_k(jax.random.fold_in(splits[10], 71), 0)
    att_v = centred(splits[2], (TOKENS, AHEADS * HEAD_DIM), 1.0, 6.0, ((0, 64), (1, 8)))
    fast_q = centred(splits[3], (TOKENS, FHEADS * FAST_D), 1.0, 6.0, ((0, 64), (1, 8)))
    fast_k = centred(splits[4], (TOKENS, FHEADS * FAST_D), 1.0, 6.0, ((0, 64), (1, 8)))
    fast_v = centred(splits[5], (TOKENS, FHEADS * FAST_D), 1.0, 6.0, ((0, 64), (1, 8)))
    learn_rates = jnp.clip(jnp.exp(math.log(0.002) - 2.3025852 * jax.random.uniform(splits[6], (TOKENS,), jnp.float32) ** shard_levels(splits[6], (TOKENS,), ((0, 64),), -0.2, 0.2)), 0.0002, 0.002)
    w_gate = centred(splits[7], (FAST_D, FHEADS * FAST_HID), FAST_D ** -0.5, 0.25, ((1, 8),))
    w_up = centred(splits[8], (FAST_D, FHEADS * FAST_HID), FAST_D ** -0.5, 0.25, ((1, 8),))
    w_down = centred(splits[9], (FAST_D, FHEADS * FAST_HID), FAST_HID ** -0.5, 0.25, ((1, 8),))
    return {"att_q": att_q, "att_k": att_k, "att_v": att_v, "fast_q": fast_q, "fast_k": fast_k, "fast_v": fast_v, "learn_rates": learn_rates, "w_gate": w_gate, "w_up": w_up, "w_down": w_down}


norm_eps = 1e-06

def silu_slope(pre_act):
    sigmoid_v = jax.nn.sigmoid(pre_act)
    return sigmoid_v * (1.0 + pre_act * (1.0 - sigmoid_v))

def window_attention(att_q, att_k, att_v):
    token_count = att_q.shape[0]
    zero_pad = jnp.zeros((WINDOW, att_k.shape[1]), att_k.dtype)
    keys_all = jnp.concatenate([zero_pad, att_k], 0)
    values_all = jnp.concatenate([zero_pad, att_v], 0)
    block_count = token_count // TOK_DEV

    def one_block(block_index):
        row_start = (block_index * TOK_DEV).astype(jnp.int32)
        query_block = lax.dynamic_slice_in_dim(att_q, row_start, TOK_DEV, 0).reshape(TOK_DEV, AHEADS, HEAD_DIM)
        key_block = lax.dynamic_slice_in_dim(keys_all, row_start, WINDOW + TOK_DEV, 0).reshape(WINDOW + TOK_DEV, AHEADS, HEAD_DIM)
        val_block = lax.dynamic_slice_in_dim(values_all, row_start, WINDOW + TOK_DEV, 0).reshape(WINDOW + TOK_DEV, AHEADS, HEAD_DIM)
        scores = jnp.einsum('qhd,khd->hqk', query_block.astype(jnp.float32), key_block.astype(jnp.float32)) * HEAD_DIM ** (-0.5)
        query_pos = row_start + jnp.arange(TOK_DEV, dtype=jnp.int32)
        key_pos = row_start - WINDOW + jnp.arange(WINDOW + TOK_DEV, dtype=jnp.int32)
        allowed = (key_pos[None, :] <= query_pos[:, None]) & (key_pos[None, :] > query_pos[:, None] - WINDOW) & (key_pos[None, :] >= 0)
        scores = jnp.where(allowed[None], scores, jnp.float32(-1e+30))
        row_max = lax.optimization_barrier(jnp.max(scores, axis=-1, keepdims=True))
        expd = jnp.exp(scores - row_max)
        softmax_w = (expd / lax.optimization_barrier(jnp.sum(expd, axis=-1, keepdims=True))).astype(jnp.bfloat16)
        result = jnp.einsum('hqk,khd->qhd', softmax_w.astype(jnp.float32), val_block.astype(jnp.float32))
        return result.reshape(TOK_DEV, AHEADS * HEAD_DIM).astype(jnp.bfloat16)
    blocks = lax.map(one_block, jnp.arange(block_count, dtype=jnp.int32))
    return blocks.reshape(token_count, AHEADS * HEAD_DIM)

def renorm(old_weights, gradient):
    old_f = old_weights.astype(jnp.float32)
    updated = old_f + gradient
    old_norm = jnp.sqrt(lax.optimization_barrier(jnp.sum(old_f * old_f, axis=0, keepdims=True)))
    new_sq = lax.optimization_barrier(jnp.sum(updated * updated, axis=0, keepdims=True))
    return (updated * (old_norm / jnp.sqrt(new_sq + norm_eps))).astype(jnp.bfloat16)

def reference(att_q, att_k, att_v, fast_q, fast_k, fast_v, learn_rates, w_gate, w_up, w_down):
    attended = window_attention(att_q, att_k, att_v)
    rate_col = learn_rates[:, None]
    outputs = []
    for fast_head in range(FHEADS):
        feat_lo = fast_head * FAST_D
        hid_lo = fast_head * FAST_HID
        key_rows = fast_k[:, feat_lo:feat_lo + FAST_D]
        val_rows = fast_v[:, feat_lo:feat_lo + FAST_D]
        query_rows = fast_q[:, feat_lo:feat_lo + FAST_D]
        gate_w = w_gate[:, hid_lo:hid_lo + FAST_HID]
        up_w = w_up[:, hid_lo:hid_lo + FAST_HID]
        down_w = w_down[:, hid_lo:hid_lo + FAST_HID]
        pre_gate = jnp.dot(key_rows, gate_w, preferred_element_type=jnp.float32)
        pre_up = jnp.dot(key_rows, up_w, preferred_element_type=jnp.float32)
        back_proj = jnp.dot(val_rows, down_w, preferred_element_type=jnp.float32)
        gate_term = (rate_col * back_proj * pre_up * silu_slope(pre_gate)).astype(jnp.bfloat16)
        up_term = (rate_col * back_proj * jax.nn.silu(pre_gate)).astype(jnp.bfloat16)
        down_term = (rate_col * jax.nn.silu(pre_gate) * pre_up).astype(jnp.bfloat16)
        grad_gate = jnp.dot(key_rows.T, gate_term, preferred_element_type=jnp.float32)
        grad_up = jnp.dot(key_rows.T, up_term, preferred_element_type=jnp.float32)
        grad_down = jnp.dot(val_rows.T, down_term, preferred_element_type=jnp.float32)
        new_gate = renorm(gate_w, grad_gate)
        new_up = renorm(up_w, grad_up)
        new_down = renorm(down_w, grad_down)
        gate_q = jnp.dot(query_rows, new_gate, preferred_element_type=jnp.float32)
        up_q = jnp.dot(query_rows, new_up, preferred_element_type=jnp.float32)
        hidden_q = (jax.nn.silu(gate_q) * up_q).astype(jnp.bfloat16)
        outputs.append(jnp.dot(hidden_q, new_down.T, preferred_element_type=jnp.float32).astype(jnp.bfloat16))
    fast_out = jnp.concatenate(outputs, axis=1)
    return (attended, fast_out)
```

```python
import functools

import jax
import jax.numpy as jnp
from jax import lax
from jax.experimental import pallas as pl
from jax.experimental.pallas import tpu as pltpu
from jax.sharding import PartitionSpec as P

HEAD_DIM = 128
BLK = 128
HOPS = 4
NORM_EPS = 1e-06
MASKED = -1e30
MESH = pl.DeviceIdType.MESH
F32 = jnp.float32
BF16 = jnp.bfloat16


def silu_parts(pre_act):
    sig = jax.nn.sigmoid(pre_act)
    return pre_act * sig, sig * (1.0 + pre_act * (1.0 - sig))


def contract_rows(lhs, rhs):
    return lax.dot_general(lhs, rhs, (((0,), (0,)), ((), ())), preferred_element_type=F32)


def contract_cols(lhs, rhs):
    return lax.dot_general(lhs, rhs, (((1,), (1,)), ((), ())), preferred_element_type=F32)


def kernel(
    ny, nz,
    aq_h, ak_h, av_h, fq_h, fk_h, fv_h, lr_h, wg_h, wu_h, wd_h,
    att_h, out_h,
    aq, okv, halo, fq, kvf, lr, w3, tt, rt, grad, ry, zs, zr, old_t, fresh,
    m_s, l_s, acc_s, att_v, out_v,
    loc, osem, hs, hr, ps, pr, ts, tr, rs_s, rs_r, zs_s, zs_r, az_s, az_r, ag_s, ag_r, ad_s, ad_r,
):
    tok, feat = aq.shape
    nb = w3.shape[2] // BLK
    heads = feat // HEAD_DIM
    half = BLK // 2
    zrow = BLK // nz
    s = lax.axis_index("seq")
    total = 2 * ny * nz
    c = lax.rem(s, 2)
    y = lax.rem(s // 2, ny)
    z = s // (2 * ny)
    mate = s + 1 - 2 * c
    y_next = z * 2 * ny + lax.rem(y + 1, ny) * 2 + c
    y_prev = z * 2 * ny + lax.rem(y + ny - 1, ny) * 2 + c
    z_peer = [lax.rem(z + i, nz) * 2 * ny + y * 2 + c for i in range(1, nz)]
    chain = {(0, 0): ny // 2, (0, 1): ny // 2 - 1, (1, 0): ny // 2 - 1, (1, 1): ny // 2}
    max_hop = ny // 2

    def remote(src, dst, ssem, rsem, dev):
        return pltpu.make_async_remote_copy(
            src_ref=src, dst_ref=dst, send_sem=ssem, recv_sem=rsem,
            device_id={"seq": dev}, device_id_type=MESH,
        )

    loads = [
        (fk_h, kvf.at[0, 0]), (wg_h, w3.at[0]), (wu_h, w3.at[1]), (lr_h, lr),
        (fv_h, kvf.at[0, 1]), (wd_h, w3.at[2]),
        (aq_h, aq), (ak_h, okv.at[0]), (av_h, okv.at[1]), (fq_h, fq),
    ]
    loads = [pltpu.make_async_copy(src, dst, loc.at[i]) for i, (src, dst) in enumerate(loads)]
    for one in loads:
        one.start()

    barrier = pltpu.get_barrier_semaphore()
    for peer in [mate, y_next, y_prev] + z_peer:
        pl.semaphore_signal(barrier, inc=1, device_id={"seq": peer}, device_id_type=MESH)

    @pl.when((c == 1) & (s < total - 1))
    def _():
        pl.semaphore_signal(barrier, inc=1, device_id={"seq": s + 1}, device_id_type=MESH)

    @pl.when((c == 0) & (s > 0))
    def _():
        pl.semaphore_signal(barrier, inc=1, device_id={"seq": s - 1}, device_id_type=MESH)

    beside = c * (1 - s // (total - 1)) + (1 - c) * ((s + total - 1) // total)
    pl.semaphore_wait(barrier, 3 + len(z_peer) + beside)

    def halo_copy(step, part, dev):
        if step == 0:
            src = (ak_h, av_h)[part]
        else:
            src = halo.at[step - 1, part]
        return remote(src, halo.at[step, part], hs.at[step, part], hr.at[step, part], dev)

    def halo_send(step):
        @pl.when((s < total - 1) & (s >= step))
        def _():
            for part in range(2):
                halo_copy(step, part, s + 1).start()

    def halo_send_wait(step):
        @pl.when((s < total - 1) & (s >= step))
        def _():
            for part in range(2):
                halo_copy(step, part, s + 1).wait_send()

    def halo_wait(step):
        @pl.when(s >= step + 1)
        def _():
            for part in range(2):
                halo_copy(step, part, s - 1).wait_recv()

    def pair_copy(part):
        return remote((fk_h, fv_h)[part], kvf.at[1, part], ps.at[part], pr.at[part], mate)

    for part in range(2):
        pair_copy(part).start()
    halo_send(0)

    scale = HEAD_DIM ** (-0.5)

    def attend(delta, lo, hi):
        def one_head(h, _):
            cols = pl.ds(pl.multiple_of(h * HEAD_DIM, HEAD_DIM), HEAD_DIM)
            kv = okv if delta == 0 else halo.at[delta - 1]
            key, val = kv[0, :, cols], kv[1, :, cols]
            sc = contract_cols(aq[:, cols], key) * scale
            if delta in (0, HOPS):
                qi = lax.broadcasted_iota(jnp.int32, (tok, tok), 0)
                ki = lax.broadcasted_iota(jnp.int32, (tok, tok), 1)
                keep = (ki <= qi) if delta == 0 else (ki > qi)
                sc = jnp.where(keep, sc, MASKED)
            top = jnp.max(sc, axis=1, keepdims=True)
            if delta == 0:
                p = jnp.exp(sc - top)
                m_s[h] = top
                l_s[h] = jnp.sum(p, axis=1, keepdims=True)
                acc_s[h] = jnp.dot(p.astype(BF16), val, preferred_element_type=F32)
            else:
                m_old = m_s[h]
                m_new = jnp.maximum(m_old, top)
                p = jnp.exp(sc - m_new)
                alpha = jnp.exp(m_old - m_new)
                m_s[h] = m_new
                l_s[h] = l_s[h] * alpha + jnp.sum(p, axis=1, keepdims=True)
                acc_s[h] = acc_s[h] * alpha + jnp.dot(p.astype(BF16), val, preferred_element_type=F32)
            return 0

        if delta == 0:
            lax.fori_loop(lo, hi, one_head, 0)
        else:
            @pl.when(s >= delta)
            def _():
                lax.fori_loop(lo, hi, one_head, 0)

    loads[0].wait()
    loads[1].wait()
    loads[2].wait()
    loads[3].wait()
    keys = kvf[0, 0]
    eye = lax.broadcasted_iota(jnp.int32, (tok, tok), 0) == lax.broadcasted_iota(jnp.int32, (tok, tok), 1)
    rate = jnp.sum(jnp.where(eye, jnp.broadcast_to(lr[...], (tok, tok)), 0.0), axis=1, keepdims=True)
    if 2 * ny > 3 * nb:
        for b in range(3 * nb, 2 * ny):
            tt[b % 2, :, (b // 2) * BLK:(b // 2 + 1) * BLK] = jnp.zeros((tok, BLK), BF16)

    def put(b, value):
        tt[b % 2, :, (b // 2) * BLK:(b // 2 + 1) * BLK] = value.astype(BF16)

    pre_gate = jnp.dot(keys, w3[0], preferred_element_type=F32)
    pre_up = jnp.dot(keys, w3[1], preferred_element_type=F32)
    loads[4].wait()
    loads[5].wait()
    back = jnp.dot(kvf[0, 1], w3[2], preferred_element_type=F32)
    for i in range(nb):
        cols = slice(i * BLK, (i + 1) * BLK)
        pg, pu, bk = pre_gate[:, cols], pre_up[:, cols], back[:, cols]
        silu, slope = silu_parts(pg)
        rb = rate * bk
        put(i, rb * pu * slope)
        put(nb + i, rb * silu)
        put(2 * nb + i, rate * silu * pu)
    term_copy = remote(tt.at[1 - c], rt, ts, tr, mate)
    term_copy.start()

    split = nb * BLK
    width = ny * BLK
    grad[0:nb] = contract_rows(tt[c, :, 0:split], kvf[0, 0]).reshape(nb, BLK, feat)
    grad[nb:ny] = contract_rows(tt[c, :, split:width], kvf[0, 1]).reshape(ny - nb, BLK, feat)
    for i in range(6, 9):
        loads[i].wait()
    attend(0, 0, heads // 2)
    term_copy.wait_recv()
    for part in range(2):
        pair_copy(part).wait_recv()
    grad[0:nb] += contract_rows(rt[:, 0:split], kvf[1, 0]).reshape(nb, BLK, feat)
    grad[nb:ny] += contract_rows(rt[:, split:width], kvf[1, 1]).reshape(ny - nb, BLK, feat)

    rows_of = [pl.ds(0, half), pl.ds(half, half)]
    slot = {}
    for way in range(2):
        for part in range(2):
            for hop in range(chain[way, part]):
                slot[way, part, hop] = len(slot)

    def toward(way, dist):
        return lax.rem(y + dist, ny) if way == 0 else lax.rem(y + ny - dist, ny)

    def rs_copy(way, part, hop):
        if hop == 0:
            src = grad.at[toward(way, chain[way, part]), rows_of[part]]
        else:
            src = ry.at[slot[way, part, hop - 1]]
        n = slot[way, part, hop]
        return remote(src, ry.at[n], rs_s.at[n], rs_r.at[n], (y_next, y_prev)[way])

    order = [(0, 0), (1, 1), (0, 1), (1, 0)]
    for way, part in order:
        if chain[way, part] > 0:
            rs_copy(way, part, 0).start()
    attend(0, heads // 2, heads)
    for hop in range(max_hop):
        for way, part in order:
            if hop >= chain[way, part]:
                continue
            rs_copy(way, part, hop).wait_recv()
            if hop + 1 < chain[way, part]:
                n = slot[way, part, hop]
                ry[n] += grad[toward(way, chain[way, part] - hop - 1), rows_of[part]]
                rs_copy(way, part, hop + 1).start()
        if hop < HOPS - 1:
            halo_wait(hop)
            halo_send(hop + 1)
            attend(hop + 1, 0, heads)
    for part in range(2):
        got = grad[y, rows_of[part]]
        for way in range(2):
            if chain[way, part] > 0:
                got += ry[slot[way, part, chain[way, part] - 1]]
        zs[rows_of[part]] = got

    def z_rows(i):
        return pl.ds(pl.multiple_of(lax.rem(z + i, nz) * zrow, zrow), zrow)

    def zs_copy(i):
        return remote(zs.at[z_rows(i)], zr.at[i - 1], zs_s.at[i - 1], zs_r.at[i - 1], z_peer[i - 1])

    for i in range(1, nz):
        zs_copy(i).start()
    own_b = 2 * y + c
    src_b = jnp.minimum(own_b, 3 * nb - 1)
    old_cols = pl.ds(pl.multiple_of(lax.rem(src_b, nb) * BLK, BLK), BLK)
    old_t[...] = w3[src_b // nb, :, old_cols].astype(F32).T
    old = old_t[z_rows(0), :]
    old_norm = jnp.sqrt(jnp.sum(old * old, axis=1, keepdims=True))
    updated = zs[z_rows(0), :]
    for i in range(1, nz):
        zs_copy(i).wait_recv()
        updated += zr[i - 1]
    updated += old
    squares = jnp.sum(updated * updated, axis=1, keepdims=True)
    fresh[own_b, z_rows(0), :] = (updated * (old_norm / jnp.sqrt(squares + NORM_EPS))).astype(BF16)

    def az_copy(i):
        here = fresh.at[own_b, z_rows(0)]
        return remote(here, here, az_s.at[i - 1], az_r.at[i - 1], z_peer[i - 1])

    for i in range(1, nz):
        az_copy(i).start()
    halo_wait(HOPS - 1)
    attend(HOPS, 0, heads // 2)
    for i in range(1, nz):
        az_copy(i).wait_recv()

    def ag_copy(way, part, hop):
        origin = toward(1 - way, hop)
        here = fresh.at[2 * origin + c, rows_of[part]]
        n = slot[way, part, hop]
        return remote(here, here, ag_s.at[n], ag_r.at[n], (y_next, y_prev)[way])

    def ag_arrival(way, part, hop):
        origin = toward(1 - way, hop + 1)
        here = fresh.at[2 * origin + c, rows_of[part]]
        n = slot[way, part, hop]
        return remote(here, here, ag_s.at[n], ag_r.at[n], (y_next, y_prev)[way])

    def ad_copy(n, origin, part):
        here = fresh.at[2 * origin + c, rows_of[part]]
        return remote(here, here, ad_s.at[n], ad_r.at[n], mate)

    for way, part in order:
        if chain[way, part] > 0:
            ag_copy(way, part, 0).start()
    passed = []
    for part in range(2):
        passed.append((y, part))
        ad_copy(len(passed) - 1, y, part).start()
    attend(HOPS, heads // 2, heads)
    for h in range(heads):
        cols = slice(h * HEAD_DIM, (h + 1) * HEAD_DIM)
        att_v[:, cols] = (acc_s[h] / l_s[h]).astype(BF16)
    att_out = pltpu.make_async_copy(att_v, att_h, osem.at[0])
    att_out.start()
    for hop in range(max_hop):
        for way, part in order:
            if hop >= chain[way, part]:
                continue
            ag_arrival(way, part, hop).wait_recv()
            if hop + 1 < chain[way, part]:
                ag_copy(way, part, hop + 1).start()
            origin = toward(1 - way, hop + 1)
            passed.append((origin, part))
            ad_copy(len(passed) - 1, origin, part).start()
    for n, (origin, part) in enumerate(passed):
        ad_copy(n, origin, part).wait_recv()

    loads[9].wait()
    hid = nb * BLK
    queries = fq[...]
    gate_q = contract_cols(queries, fresh[0:nb].reshape(hid, feat))
    up_q = contract_cols(queries, fresh[nb:2 * nb].reshape(hid, feat))
    hidden = (jax.nn.silu(gate_q) * up_q).astype(BF16)
    out_v[...] = jnp.dot(
        hidden, fresh[2 * nb:3 * nb].reshape(hid, feat), preferred_element_type=F32
    ).astype(BF16)
    fast_out = pltpu.make_async_copy(out_v, out_h, osem.at[1])
    fast_out.start()

    for step in range(HOPS):
        halo_send_wait(step)
    for part in range(2):
        pair_copy(part).wait_send()
    term_copy.wait_send()
    for way, part, hop in slot:
        rs_copy(way, part, hop).wait_send()
        ag_copy(way, part, hop).wait_send()
    for i in range(1, nz):
        zs_copy(i).wait_send()
        az_copy(i).wait_send()
    for n, (origin, part) in enumerate(passed):
        ad_copy(n, origin, part).wait_send()
    att_out.wait()
    fast_out.wait()


def solution(mesh):
    nz = 4 if mesh.shape["seq"] == 64 else 2
    ny = mesh.shape["seq"] // (2 * nz)

    def body(att_q, att_k, att_v, fast_q, fast_k, fast_v, rates, w_gate, w_up, w_down):
        tok, feat = att_q.shape
        hid = w_gate.shape[1]
        heads = feat // HEAD_DIM
        n_slot = 2 * (ny - 1)
        dma = pltpu.SemaphoreType.DMA
        vmem = pltpu.VMEM
        hbm = pl.BlockSpec(memory_space=pl.ANY)
        return pl.pallas_call(
            functools.partial(kernel, ny, nz),
            out_shape=(
                jax.ShapeDtypeStruct((tok, feat), BF16),
                jax.ShapeDtypeStruct((tok, feat), BF16),
            ),
            in_specs=[hbm] * 10,
            out_specs=(hbm, hbm),
            scratch_shapes=[
                vmem((tok, feat), BF16),
                vmem((2, tok, feat), BF16),
                vmem((HOPS, 2, tok, feat), BF16),
                vmem((tok, feat), BF16),
                vmem((2, 2, tok, feat), BF16),
                vmem((1, tok), F32),
                vmem((3, feat, hid), BF16),
                vmem((2, tok, ny * BLK), BF16),
                vmem((tok, ny * BLK), BF16),
                vmem((ny, BLK, feat), F32),
                vmem((n_slot, BLK // 2, feat), F32),
                vmem((BLK, feat), F32),
                vmem((nz - 1, BLK // nz, feat), F32),
                vmem((BLK, feat), F32),
                vmem((2 * ny, BLK, feat), BF16),
                vmem((heads, tok, 1), F32),
                vmem((heads, tok, 1), F32),
                vmem((heads, tok, HEAD_DIM), F32),
                vmem((tok, feat), BF16),
                vmem((tok, feat), BF16),
                dma((10,)),
                dma((2,)),
                dma((HOPS, 2)),
                dma((HOPS, 2)),
                dma((2,)),
                dma((2,)),
                dma,
                dma,
                dma((n_slot,)),
                dma((n_slot,)),
                dma((nz - 1,)),
                dma((nz - 1,)),
                dma((nz - 1,)),
                dma((nz - 1,)),
                dma((n_slot,)),
                dma((n_slot,)),
                dma((2 * ny,)),
                dma((2 * ny,)),
            ],
            compiler_params=pltpu.CompilerParams(
                collective_id=0, has_side_effects=True, vmem_limit_bytes=60 * 1024 * 1024
            ),
        )(
            att_q, att_k, att_v, fast_q, fast_k, fast_v, rates.reshape(1, -1),
            w_gate, w_up, w_down,
        )

    rows = P("seq", "head")
    weights = P(None, "head")
    return jax.shard_map(
        body,
        mesh=mesh,
        in_specs=(rows,) * 6 + (P("seq"),) + (weights,) * 3,
        out_specs=(rows, rows),
        check_vma=False,
    )
```

```python
import functools

import jax
import jax.numpy as jnp
from jax import lax
from jax.experimental import pallas as pl
from jax.experimental.pallas import tpu as pltpu
from jax.sharding import PartitionSpec as P

HEAD_DIM = 128
BLK = 128
HOPS = 4
NORM_EPS = 1e-06
MASKED = -1e30
MESH = pl.DeviceIdType.MESH
F32 = jnp.float32
BF16 = jnp.bfloat16


def silu_parts(pre_act):
    sig = jax.nn.sigmoid(pre_act)
    return pre_act * sig, sig * (1.0 + pre_act * (1.0 - sig))


def contract_rows(lhs, rhs):
    return lax.dot_general(lhs, rhs, (((0,), (0,)), ((), ())), preferred_element_type=F32)


def contract_cols(lhs, rhs):
    return lax.dot_general(lhs, rhs, (((1,), (1,)), ((), ())), preferred_element_type=F32)


def kernel(
    ny, nz,
    aq_h, ak_h, av_h, fq_h, fk_h, fv_h, lr_h, wg_h, wu_h, wd_h,
    att_h, out_h,
    aq, okv, halo, fq, kvf, lr, w3, tt, rt, grad, ry, zs, zr, old_t, fresh,
    m_s, l_s, acc_s, att_v, out_v,
    loc, osem, hs, hr, ps, pr, ts, tr, rs_s, rs_r, zs_s, zs_r, az_s, az_r, ag_s, ag_r, ad_s, ad_r,
):
    tok, feat = aq.shape
    nb = w3.shape[2] // BLK
    heads = feat // HEAD_DIM
    half = BLK // 2
    zrow = BLK // nz
    s = lax.axis_index("seq")
    total = 2 * ny * nz
    c = lax.rem(s, 2)
    y = lax.rem(s // 2, ny)
    z = s // (2 * ny)
    mate = s + 1 - 2 * c
    y_next = z * 2 * ny + lax.rem(y + 1, ny) * 2 + c
    y_prev = z * 2 * ny + lax.rem(y + ny - 1, ny) * 2 + c
    z_peer = [lax.rem(z + i, nz) * 2 * ny + y * 2 + c for i in range(1, nz)]
    lean = max(ny // 4, 1)
    chain = {(0, 0): lean, (0, 1): lean + 1, (1, 0): ny - 1 - lean, (1, 1): ny - 2 - lean}
    even = {(0, 0): ny // 2, (0, 1): ny // 2 - 1, (1, 0): ny // 2 - 1, (1, 1): ny // 2}

    def remote(src, dst, ssem, rsem, dev):
        return pltpu.make_async_remote_copy(
            src_ref=src, dst_ref=dst, send_sem=ssem, recv_sem=rsem,
            device_id={"seq": dev}, device_id_type=MESH,
        )

    loads = [
        (fk_h, kvf.at[0, 0]), (wg_h, w3.at[0]), (wu_h, w3.at[1]), (lr_h, lr),
        (fv_h, kvf.at[0, 1]), (wd_h, w3.at[2]),
        (aq_h, aq), (ak_h, okv.at[0]), (av_h, okv.at[1]), (fq_h, fq),
    ]
    loads = [pltpu.make_async_copy(src, dst, loc.at[i]) for i, (src, dst) in enumerate(loads)]
    for one in loads:
        one.start()

    barrier = pltpu.get_barrier_semaphore()
    for peer in [mate, y_next, y_prev] + z_peer:
        pl.semaphore_signal(barrier, inc=1, device_id={"seq": peer}, device_id_type=MESH)

    @pl.when((c == 1) & (s < total - 1))
    def _():
        pl.semaphore_signal(barrier, inc=1, device_id={"seq": s + 1}, device_id_type=MESH)

    @pl.when((c == 0) & (s > 0))
    def _():
        pl.semaphore_signal(barrier, inc=1, device_id={"seq": s - 1}, device_id_type=MESH)

    beside = c * (1 - s // (total - 1)) + (1 - c) * ((s + total - 1) // total)
    pl.semaphore_wait(barrier, 3 + len(z_peer) + beside)

    def halo_copy(step, part, dev):
        if step == 0:
            src = (ak_h, av_h)[part]
        else:
            src = halo.at[step - 1, part]
        return remote(src, halo.at[step, part], hs.at[step, part], hr.at[step, part], dev)

    def halo_send(step):
        @pl.when((s < total - 1) & (s >= step))
        def _():
            for part in range(2):
                halo_copy(step, part, s + 1).start()

    def halo_send_wait(step):
        @pl.when((s < total - 1) & (s >= step))
        def _():
            for part in range(2):
                halo_copy(step, part, s + 1).wait_send()

    def halo_wait(step):
        @pl.when(s >= step + 1)
        def _():
            for part in range(2):
                halo_copy(step, part, s - 1).wait_recv()

    def pair_copy(part):
        return remote((fk_h, fv_h)[part], kvf.at[1, part], ps.at[part], pr.at[part], mate)

    for part in range(2):
        pair_copy(part).start()
    halo_send(0)

    scale = HEAD_DIM ** (-0.5)

    def attend(delta, lo, hi):
        def one_head(h, _):
            cols = pl.ds(pl.multiple_of(h * HEAD_DIM, HEAD_DIM), HEAD_DIM)
            kv = okv if delta == 0 else halo.at[delta - 1]
            key, val = kv[0, :, cols], kv[1, :, cols]
            sc = contract_cols(aq[:, cols], key) * scale
            if delta in (0, HOPS):
                qi = lax.broadcasted_iota(jnp.int32, (tok, tok), 0)
                ki = lax.broadcasted_iota(jnp.int32, (tok, tok), 1)
                keep = (ki <= qi) if delta == 0 else (ki > qi)
                sc = jnp.where(keep, sc, MASKED)
            top = jnp.max(sc, axis=1, keepdims=True)
            if delta == 0:
                p = jnp.exp(sc - top)
                m_s[h] = top
                l_s[h] = jnp.sum(p, axis=1, keepdims=True)
                acc_s[h] = jnp.dot(p.astype(BF16), val, preferred_element_type=F32)
            else:
                m_old = m_s[h]
                m_new = jnp.maximum(m_old, top)
                p = jnp.exp(sc - m_new)
                alpha = jnp.exp(m_old - m_new)
                m_s[h] = m_new
                l_s[h] = l_s[h] * alpha + jnp.sum(p, axis=1, keepdims=True)
                acc_s[h] = acc_s[h] * alpha + jnp.dot(p.astype(BF16), val, preferred_element_type=F32)
            return 0

        if delta == 0:
            lax.fori_loop(lo, hi, one_head, 0)
        else:
            @pl.when(s >= delta)
            def _():
                lax.fori_loop(lo, hi, one_head, 0)

    loads[0].wait()
    loads[1].wait()
    loads[2].wait()
    loads[3].wait()
    keys = kvf[0, 0]
    eye = lax.broadcasted_iota(jnp.int32, (tok, tok), 0) == lax.broadcasted_iota(jnp.int32, (tok, tok), 1)
    rate = jnp.sum(jnp.where(eye, jnp.broadcast_to(lr[...], (tok, tok)), 0.0), axis=1, keepdims=True)
    if 2 * ny > 3 * nb:
        for b in range(3 * nb, 2 * ny):
            tt[b % 2, :, (b // 2) * BLK:(b // 2 + 1) * BLK] = jnp.zeros((tok, BLK), BF16)

    def put(b, value):
        tt[b % 2, :, (b // 2) * BLK:(b // 2 + 1) * BLK] = value.astype(BF16)

    pre_gate = jnp.dot(keys, w3[0], preferred_element_type=F32)
    pre_up = jnp.dot(keys, w3[1], preferred_element_type=F32)
    loads[4].wait()
    loads[5].wait()
    back = jnp.dot(kvf[0, 1], w3[2], preferred_element_type=F32)
    for i in range(nb):
        cols = slice(i * BLK, (i + 1) * BLK)
        pg, pu, bk = pre_gate[:, cols], pre_up[:, cols], back[:, cols]
        silu, slope = silu_parts(pg)
        rb = rate * bk
        put(i, rb * pu * slope)
        put(nb + i, rb * silu)
        put(2 * nb + i, rate * silu * pu)
    term_copy = remote(tt.at[1 - c], rt, ts, tr, mate)
    term_copy.start()

    split = nb * BLK
    width = ny * BLK
    grad[0:nb] = contract_rows(tt[c, :, 0:split], kvf[0, 0]).reshape(nb, BLK, feat)
    grad[nb:ny] = contract_rows(tt[c, :, split:width], kvf[0, 1]).reshape(ny - nb, BLK, feat)
    for i in range(6, 9):
        loads[i].wait()
    attend(0, 0, heads // 2)
    term_copy.wait_recv()
    for part in range(2):
        pair_copy(part).wait_recv()
    grad[0:nb] += contract_rows(rt[:, 0:split], kvf[1, 0]).reshape(nb, BLK, feat)
    grad[nb:ny] += contract_rows(rt[:, split:width], kvf[1, 1]).reshape(ny - nb, BLK, feat)

    rows_of = [pl.ds(0, half), pl.ds(half, half)]
    slot, ag_slot = {}, {}
    for way in range(2):
        for part in range(2):
            for hop in range(chain[way, part]):
                slot[way, part, hop] = len(slot)
            for hop in range(even[way, part]):
                ag_slot[way, part, hop] = len(ag_slot)

    def toward(way, dist):
        return lax.rem(y + dist, ny) if way == 0 else lax.rem(y + ny - dist, ny)

    def rs_copy(way, part, hop):
        if hop == 0:
            src = grad.at[toward(way, chain[way, part]), rows_of[part]]
        else:
            src = ry.at[slot[way, part, hop - 1]]
        n = slot[way, part, hop]
        return remote(src, ry.at[n], rs_s.at[n], rs_r.at[n], (y_next, y_prev)[way])

    @pl.when(c == 1)
    def _():
        halo_wait(0)
        halo_send(1)

    order = [(1, 0), (0, 1), (1, 1), (0, 0)]
    for way, part in order:
        if chain[way, part] > 0:
            rs_copy(way, part, 0).start()
    attend(0, heads // 2, heads)

    @pl.when(c == 0)
    def _():
        halo_wait(0)
        halo_send(1)

    for hop in range(max(chain.values())):
        for way, part in order:
            if hop >= chain[way, part]:
                continue
            rs_copy(way, part, hop).wait_recv()
            if hop + 1 < chain[way, part]:
                n = slot[way, part, hop]
                ry[n] += grad[toward(way, chain[way, part] - hop - 1), rows_of[part]]
                rs_copy(way, part, hop + 1).start()
        if hop == 0:
            attend(1, 0, heads)
        elif hop < HOPS - 1:
            halo_wait(hop)
            halo_send(hop + 1)
            attend(hop + 1, 0, heads)
    for part in range(2):
        got = grad[y, rows_of[part]]
        for way in range(2):
            if chain[way, part] > 0:
                got += ry[slot[way, part, chain[way, part] - 1]]
        zs[rows_of[part]] = got

    def z_rows(i):
        return pl.ds(pl.multiple_of(lax.rem(z + i, nz) * zrow, zrow), zrow)

    def zs_copy(i):
        return remote(zs.at[z_rows(i)], zr.at[i - 1], zs_s.at[i - 1], zs_r.at[i - 1], z_peer[i - 1])

    for i in range(1, nz):
        zs_copy(i).start()
    own_b = 2 * y + c
    src_b = jnp.minimum(own_b, 3 * nb - 1)
    old_cols = pl.ds(pl.multiple_of(lax.rem(src_b, nb) * BLK, BLK), BLK)
    old_t[...] = w3[src_b // nb, :, old_cols].astype(F32).T
    old = old_t[z_rows(0), :]
    old_norm = jnp.sqrt(jnp.sum(old * old, axis=1, keepdims=True))
    updated = zs[z_rows(0), :]
    for i in range(1, nz):
        zs_copy(i).wait_recv()
        updated += zr[i - 1]
    updated += old
    squares = jnp.sum(updated * updated, axis=1, keepdims=True)
    fresh[own_b, z_rows(0), :] = (updated * (old_norm / jnp.sqrt(squares + NORM_EPS))).astype(BF16)

    def az_copy(i):
        here = fresh.at[own_b, z_rows(0)]
        return remote(here, here, az_s.at[i - 1], az_r.at[i - 1], z_peer[i - 1])

    for i in range(1, nz):
        az_copy(i).start()
    halo_wait(HOPS - 1)
    attend(HOPS, 0, heads // 2)
    for i in range(1, nz):
        az_copy(i).wait_recv()

    def ag_copy(way, part, hop):
        origin = toward(1 - way, hop)
        here = fresh.at[2 * origin + c, rows_of[part]]
        n = ag_slot[way, part, hop]
        return remote(here, here, ag_s.at[n], ag_r.at[n], (y_next, y_prev)[way])

    def ag_arrival(way, part, hop):
        origin = toward(1 - way, hop + 1)
        here = fresh.at[2 * origin + c, rows_of[part]]
        n = ag_slot[way, part, hop]
        return remote(here, here, ag_s.at[n], ag_r.at[n], (y_next, y_prev)[way])

    def ad_copy(n, origin, part):
        here = fresh.at[2 * origin + c, rows_of[part]]
        return remote(here, here, ad_s.at[n], ad_r.at[n], mate)

    for way, part in even:
        if even[way, part] > 0:
            ag_copy(way, part, 0).start()
    passed = []
    for part in range(2):
        passed.append((y, part))
        ad_copy(len(passed) - 1, y, part).start()
    attend(HOPS, heads // 2, heads)
    for h in range(heads):
        cols = slice(h * HEAD_DIM, (h + 1) * HEAD_DIM)
        att_v[:, cols] = (acc_s[h] / l_s[h]).astype(BF16)
    att_out = pltpu.make_async_copy(att_v, att_h, osem.at[0])
    att_out.start()
    for hop in range(ny // 2):
        for way, part in even:
            if hop >= even[way, part]:
                continue
            ag_arrival(way, part, hop).wait_recv()
            if hop + 1 < even[way, part]:
                ag_copy(way, part, hop + 1).start()
            origin = toward(1 - way, hop + 1)
            passed.append((origin, part))
            ad_copy(len(passed) - 1, origin, part).start()
    for n, (origin, part) in enumerate(passed):
        ad_copy(n, origin, part).wait_recv()

    loads[9].wait()
    hid = nb * BLK
    queries = fq[...]
    gate_q = contract_cols(queries, fresh[0:nb].reshape(hid, feat))
    up_q = contract_cols(queries, fresh[nb:2 * nb].reshape(hid, feat))
    hidden = (jax.nn.silu(gate_q) * up_q).astype(BF16)
    out_v[...] = jnp.dot(
        hidden, fresh[2 * nb:3 * nb].reshape(hid, feat), preferred_element_type=F32
    ).astype(BF16)
    fast_out = pltpu.make_async_copy(out_v, out_h, osem.at[1])
    fast_out.start()

    for step in range(HOPS):
        halo_send_wait(step)
    for part in range(2):
        pair_copy(part).wait_send()
    term_copy.wait_send()
    for way, part, hop in slot:
        rs_copy(way, part, hop).wait_send()
    for way, part, hop in ag_slot:
        ag_copy(way, part, hop).wait_send()
    for i in range(1, nz):
        zs_copy(i).wait_send()
        az_copy(i).wait_send()
    for n, (origin, part) in enumerate(passed):
        ad_copy(n, origin, part).wait_send()
    att_out.wait()
    fast_out.wait()


def solution(mesh):
    nz = 4 if mesh.shape["seq"] == 64 else 2
    ny = mesh.shape["seq"] // (2 * nz)

    def body(att_q, att_k, att_v, fast_q, fast_k, fast_v, rates, w_gate, w_up, w_down):
        tok, feat = att_q.shape
        hid = w_gate.shape[1]
        heads = feat // HEAD_DIM
        n_slot = 2 * (ny - 1)
        dma = pltpu.SemaphoreType.DMA
        vmem = pltpu.VMEM
        hbm = pl.BlockSpec(memory_space=pl.ANY)
        return pl.pallas_call(
            functools.partial(kernel, ny, nz),
            out_shape=(
                jax.ShapeDtypeStruct((tok, feat), BF16),
                jax.ShapeDtypeStruct((tok, feat), BF16),
            ),
            in_specs=[hbm] * 10,
            out_specs=(hbm, hbm),
            scratch_shapes=[
                vmem((tok, feat), BF16),
                vmem((2, tok, feat), BF16),
                vmem((HOPS, 2, tok, feat), BF16),
                vmem((tok, feat), BF16),
                vmem((2, 2, tok, feat), BF16),
                vmem((1, tok), F32),
                vmem((3, feat, hid), BF16),
                vmem((2, tok, ny * BLK), BF16),
                vmem((tok, ny * BLK), BF16),
                vmem((ny, BLK, feat), F32),
                vmem((n_slot, BLK // 2, feat), F32),
                vmem((BLK, feat), F32),
                vmem((nz - 1, BLK // nz, feat), F32),
                vmem((BLK, feat), F32),
                vmem((2 * ny, BLK, feat), BF16),
                vmem((heads, tok, 1), F32),
                vmem((heads, tok, 1), F32),
                vmem((heads, tok, HEAD_DIM), F32),
                vmem((tok, feat), BF16),
                vmem((tok, feat), BF16),
                dma((10,)),
                dma((2,)),
                dma((HOPS, 2)),
                dma((HOPS, 2)),
                dma((2,)),
                dma((2,)),
                dma,
                dma,
                dma((n_slot,)),
                dma((n_slot,)),
                dma((nz - 1,)),
                dma((nz - 1,)),
                dma((nz - 1,)),
                dma((nz - 1,)),
                dma((n_slot,)),
                dma((n_slot,)),
                dma((2 * ny,)),
                dma((2 * ny,)),
            ],
            compiler_params=pltpu.CompilerParams(
                collective_id=0, has_side_effects=True, vmem_limit_bytes=60 * 1024 * 1024
            ),
        )(
            att_q, att_k, att_v, fast_q, fast_k, fast_v, rates.reshape(1, -1),
            w_gate, w_up, w_down,
        )

    rows = P("seq", "head")
    weights = P(None, "head")
    return jax.shard_map(
        body,
        mesh=mesh,
        in_specs=(rows,) * 6 + (P("seq"),) + (weights,) * 3,
        out_specs=(rows, rows),
        check_vma=False,
    )
```

```python
import functools

import jax
import jax.numpy as jnp
from jax import lax
from jax.experimental import pallas as pl
from jax.experimental.pallas import tpu as pltpu
from jax.sharding import PartitionSpec as P

HEAD_DIM = 128
BLK = 128
HOPS = 4
RS_Z = 256
AG_Z = 128
NORM_EPS = 1e-06
MASKED = -1e30
MESH = pl.DeviceIdType.MESH
F32 = jnp.float32
BF16 = jnp.bfloat16


def silu_parts(pre_act):
    sig = jax.nn.sigmoid(pre_act)
    return pre_act * sig, sig * (1.0 + pre_act * (1.0 - sig))


def contract_rows(lhs, rhs):
    return lax.dot_general(lhs, rhs, (((0,), (0,)), ((), ())), preferred_element_type=F32)


def contract_cols(lhs, rhs):
    return lax.dot_general(lhs, rhs, (((1,), (1,)), ((), ())), preferred_element_type=F32)


def kernel(
    ny, nz, rs_lanes, ag_lanes,
    aq_h, ak_h, av_h, fq_h, fk_h, fv_h, lr_h, wg_h, wu_h, wd_h,
    att_h, out_h,
    aq, okv, halo, fq, kvf, lr, w3, tt, rt, grad, ry, zs, zr, old_t, fresh,
    g_z, gb_z, in_z, q_z, qb_z, in_y, fresh_z,
    m_s, l_s, acc_s, att_v, out_v,
    loc, osem, hs, hr, ps, pr, ts, tr, rs_s, rs_r, zs_s, zs_r, az_s, az_r, ag_s, ag_r, ad_s, ad_r,
    zz_s, zz_r, zy_s, zy_r, by_s, by_r, bz_s, bz_r, bd_s, bd_r,
):
    tok, feat = aq.shape
    nb = w3.shape[2] // BLK
    heads = feat // HEAD_DIM
    half = BLK // 2
    zrow = BLK // nz
    s = lax.axis_index("seq")
    total = 2 * ny * nz
    c = lax.rem(s, 2)
    y = lax.rem(s // 2, ny)
    z = s // (2 * ny)
    mate = s + 1 - 2 * c
    y_next = z * 2 * ny + lax.rem(y + 1, ny) * 2 + c
    y_prev = z * 2 * ny + lax.rem(y + ny - 1, ny) * 2 + c
    y_peer = [z * 2 * ny + lax.rem(y + k, ny) * 2 + c for k in range(1, ny)]
    z_peer = [lax.rem(z + i, nz) * 2 * ny + y * 2 + c for i in range(1, nz)]
    lean = max(ny // 4, 1)
    chain = {(0, 0): lean, (0, 1): lean + 1, (1, 0): ny - 1 - lean, (1, 1): ny - 2 - lean}
    even = {(0, 0): ny // 2, (0, 1): ny // 2 - 1, (1, 0): ny // 2 - 1, (1, 1): ny // 2}

    def remote(src, dst, ssem, rsem, dev):
        return pltpu.make_async_remote_copy(
            src_ref=src, dst_ref=dst, send_sem=ssem, recv_sem=rsem,
            device_id={"seq": dev}, device_id_type=MESH,
        )

    loads = [
        (fk_h, kvf.at[0, 0]), (wg_h, w3.at[0]), (wu_h, w3.at[1]), (lr_h, lr),
        (fv_h, kvf.at[0, 1]), (wd_h, w3.at[2]),
        (aq_h, aq), (ak_h, okv.at[0]), (av_h, okv.at[1]), (fq_h, fq),
    ]
    loads = [pltpu.make_async_copy(src, dst, loc.at[i]) for i, (src, dst) in enumerate(loads)]
    for one in loads:
        one.start()

    barrier = pltpu.get_barrier_semaphore()
    for peer in [mate] + y_peer + z_peer:
        pl.semaphore_signal(barrier, inc=1, device_id={"seq": peer}, device_id_type=MESH)

    @pl.when((c == 1) & (s < total - 1))
    def _():
        pl.semaphore_signal(barrier, inc=1, device_id={"seq": s + 1}, device_id_type=MESH)

    @pl.when((c == 0) & (s > 0))
    def _():
        pl.semaphore_signal(barrier, inc=1, device_id={"seq": s - 1}, device_id_type=MESH)

    beside = c * (1 - s // (total - 1)) + (1 - c) * ((s + total - 1) // total)
    pl.semaphore_wait(barrier, 1 + len(y_peer) + len(z_peer) + beside)

    def halo_copy(step, part, dev):
        if step == 0:
            src = (ak_h, av_h)[part]
        else:
            src = halo.at[step - 1, part]
        return remote(src, halo.at[step, part], hs.at[step, part], hr.at[step, part], dev)

    def halo_send(step):
        @pl.when((s < total - 1) & (s >= step))
        def _():
            for part in range(2):
                halo_copy(step, part, s + 1).start()

    def halo_send_wait(step):
        @pl.when((s < total - 1) & (s >= step))
        def _():
            for part in range(2):
                halo_copy(step, part, s + 1).wait_send()

    def halo_wait(step):
        @pl.when(s >= step + 1)
        def _():
            for part in range(2):
                halo_copy(step, part, s - 1).wait_recv()

    def pair_copy(part):
        return remote((fk_h, fv_h)[part], kvf.at[1, part], ps.at[part], pr.at[part], mate)

    for part in range(2):
        pair_copy(part).start()
    halo_send(0)

    scale = HEAD_DIM ** (-0.5)

    def attend(delta, lo, hi):
        def one_head(h, _):
            cols = pl.ds(pl.multiple_of(h * HEAD_DIM, HEAD_DIM), HEAD_DIM)
            kv = okv if delta == 0 else halo.at[delta - 1]
            key, val = kv[0, :, cols], kv[1, :, cols]
            sc = contract_cols(aq[:, cols], key) * scale
            if delta in (0, HOPS):
                qi = lax.broadcasted_iota(jnp.int32, (tok, tok), 0)
                ki = lax.broadcasted_iota(jnp.int32, (tok, tok), 1)
                keep = (ki <= qi) if delta == 0 else (ki > qi)
                sc = jnp.where(keep, sc, MASKED)
            top = jnp.max(sc, axis=1, keepdims=True)
            if delta == 0:
                p = jnp.exp(sc - top)
                m_s[h] = top
                l_s[h] = jnp.sum(p, axis=1, keepdims=True)
                acc_s[h] = jnp.dot(p.astype(BF16), val, preferred_element_type=F32)
            else:
                m_old = m_s[h]
                m_new = jnp.maximum(m_old, top)
                p = jnp.exp(sc - m_new)
                alpha = jnp.exp(m_old - m_new)
                m_s[h] = m_new
                l_s[h] = l_s[h] * alpha + jnp.sum(p, axis=1, keepdims=True)
                acc_s[h] = acc_s[h] * alpha + jnp.dot(p.astype(BF16), val, preferred_element_type=F32)
            return 0

        if delta == 0:
            lax.fori_loop(lo, hi, one_head, 0)
        else:
            @pl.when(s >= delta)
            def _():
                lax.fori_loop(lo, hi, one_head, 0)

    loads[0].wait()
    loads[1].wait()
    loads[2].wait()
    loads[3].wait()
    keys = kvf[0, 0]
    eye = lax.broadcasted_iota(jnp.int32, (tok, tok), 0) == lax.broadcasted_iota(jnp.int32, (tok, tok), 1)
    rate = jnp.sum(jnp.where(eye, jnp.broadcast_to(lr[...], (tok, tok)), 0.0), axis=1, keepdims=True)
    if 2 * ny > 3 * nb:
        for b in range(3 * nb, 2 * ny):
            tt[b % 2, :, (b // 2) * BLK:(b // 2 + 1) * BLK] = jnp.zeros((tok, BLK), BF16)

    def put(b, value):
        tt[b % 2, :, (b // 2) * BLK:(b // 2 + 1) * BLK] = value.astype(BF16)

    pre_gate = jnp.dot(keys, w3[0], preferred_element_type=F32)
    pre_up = jnp.dot(keys, w3[1], preferred_element_type=F32)
    loads[4].wait()
    loads[5].wait()
    back = jnp.dot(kvf[0, 1], w3[2], preferred_element_type=F32)
    for i in range(nb):
        cols = slice(i * BLK, (i + 1) * BLK)
        pg, pu, bk = pre_gate[:, cols], pre_up[:, cols], back[:, cols]
        silu, slope = silu_parts(pg)
        rb = rate * bk
        put(i, rb * pu * slope)
        put(nb + i, rb * silu)
        put(2 * nb + i, rate * silu * pu)
    term_copy = remote(tt.at[1 - c], rt, ts, tr, mate)
    term_copy.start()

    split = nb * BLK
    width = ny * BLK
    lanes_y, lanes_z = pl.ds(0, rs_lanes), pl.ds(rs_lanes, feat - rs_lanes)

    def add_grads(terms, side, lanes, into, first):
        low = contract_rows(terms(0, split), kvf[side, 0, :, lanes]).reshape(nb, BLK, -1)
        high = contract_rows(terms(split, width), kvf[side, 1, :, lanes]).reshape(ny - nb, BLK, -1)
        if first:
            into[0:nb], into[nb:ny] = low, high
        else:
            into[0:nb] += low
            into[nb:ny] += high

    def own_terms(lo, hi):
        return tt[c, :, lo:hi]

    def mate_terms(lo, hi):
        return rt[:, lo:hi]

    add_grads(own_terms, 0, lanes_z, g_z, True)
    add_grads(own_terms, 0, lanes_y, grad, True)
    for i in range(6, 9):
        loads[i].wait()
    term_copy.wait_recv()
    for part in range(2):
        pair_copy(part).wait_recv()
    add_grads(mate_terms, 1, lanes_z, g_z, False)

    def z_rows(i):
        return pl.ds(pl.multiple_of(lax.rem(z + i, nz) * zrow, zrow), zrow)

    gb_z[...] = g_z[...].astype(BF16)

    def zz_copy(i):
        return remote(gb_z.at[:, z_rows(i)], in_z.at[i - 1], zz_s.at[i - 1], zz_r.at[i - 1], z_peer[i - 1])

    def zy_copy(k):
        return remote(
            qb_z.at[lax.rem(y + k, ny)], in_y.at[k - 1], zy_s.at[k - 1], zy_r.at[k - 1], y_peer[k - 1]
        )

    for i in range(1, nz):
        zz_copy(i).start()
    add_grads(mate_terms, 1, lanes_y, grad, False)

    def turn_z():
        got = g_z[:, z_rows(0), :]
        for i in range(1, nz):
            zz_copy(i).wait_recv()
            got += in_z[i - 1].astype(F32)
        q_z[...] = got
        qb_z[...] = got.astype(BF16)
        for k in range(1, ny):
            zy_copy(k).start()

    rows_of = [pl.ds(0, half), pl.ds(half, half)]
    slot, ag_slot = {}, {}
    for way in range(2):
        for part in range(2):
            for hop in range(chain[way, part]):
                slot[way, part, hop] = len(slot)
            for hop in range(even[way, part]):
                ag_slot[way, part, hop] = len(ag_slot)

    def toward(way, dist):
        return lax.rem(y + dist, ny) if way == 0 else lax.rem(y + ny - dist, ny)

    def rs_copy(way, part, hop):
        if hop == 0:
            src = grad.at[toward(way, chain[way, part]), rows_of[part]]
        else:
            src = ry.at[slot[way, part, hop - 1]]
        n = slot[way, part, hop]
        return remote(src, ry.at[n], rs_s.at[n], rs_r.at[n], (y_next, y_prev)[way])

    @pl.when(c == 1)
    def _():
        halo_wait(0)
        halo_send(1)

    order = [(1, 0), (0, 1), (1, 1), (0, 0)]
    for way, part in order:
        if chain[way, part] > 0:
            rs_copy(way, part, 0).start()
    attend(0, 0, heads)

    @pl.when(c == 0)
    def _():
        halo_wait(0)
        halo_send(1)

    for hop in range(max(chain.values())):
        for way, part in order:
            if hop >= chain[way, part]:
                continue
            rs_copy(way, part, hop).wait_recv()
            if hop + 1 < chain[way, part]:
                n = slot[way, part, hop]
                ry[n] += grad[toward(way, chain[way, part] - hop - 1), rows_of[part]]
                rs_copy(way, part, hop + 1).start()
        if hop == min(2, max(chain.values()) - 1):
            turn_z()
        if hop == 0:
            attend(1, 0, heads)
        elif hop < HOPS - 1:
            halo_wait(hop)
            halo_send(hop + 1)
            attend(hop + 1, 0, heads)
    for part in range(2):
        got = grad[y, rows_of[part]]
        for way in range(2):
            if chain[way, part] > 0:
                got += ry[slot[way, part, chain[way, part] - 1]]
        zs[rows_of[part]] = got

    def zs_copy(i):
        return remote(zs.at[z_rows(i)], zr.at[i - 1], zs_s.at[i - 1], zs_r.at[i - 1], z_peer[i - 1])

    for i in range(1, nz):
        zs_copy(i).start()
    own_b = 2 * y + c
    src_b = jnp.minimum(own_b, 3 * nb - 1)
    old_cols = pl.ds(pl.multiple_of(lax.rem(src_b, nb) * BLK, BLK), BLK)
    old_t[...] = w3[src_b // nb, :, old_cols].astype(F32).T
    old = old_t[z_rows(0), :]
    old_norm = jnp.sqrt(jnp.sum(old * old, axis=1, keepdims=True))
    sum_z = q_z[y]
    for k in range(1, ny):
        zy_copy(k).wait_recv()
        sum_z += in_y[k - 1].astype(F32)
    sum_y = zs[z_rows(0), :]
    for i in range(1, nz):
        zs_copy(i).wait_recv()
        sum_y += zr[i - 1]
    updated = old + jnp.concatenate([sum_y, sum_z], axis=1)
    squares = jnp.sum(updated * updated, axis=1, keepdims=True)
    new = (updated * (old_norm / jnp.sqrt(squares + NORM_EPS))).astype(BF16)
    fresh[c, y, z_rows(0), :] = new[:, :ag_lanes]
    fresh_z[c, y, z_rows(0), :] = new[:, ag_lanes:]

    def by_copy(k, arrival):
        here = fresh_z.at[c, lax.rem(y + ny - k, ny) if arrival else y, z_rows(0)]
        return remote(here, here, by_s.at[k - 1], by_r.at[k - 1], y_peer[k - 1])

    def bz_copy(i, arrival):
        here = fresh_z.at[c, :, z_rows(nz - i) if arrival else z_rows(0)]
        return remote(here, here, bz_s.at[i - 1], bz_r.at[i - 1], z_peer[i - 1])

    def bd_copy(i, arrival):
        here = fresh_z.at[1 - c if arrival else c, :, z_rows(nz - i)]
        return remote(here, here, bd_s.at[i], bd_r.at[i], mate)

    def az_copy(i, arrival):
        here = fresh.at[c, y, z_rows(nz - i) if arrival else z_rows(0)]
        return remote(here, here, az_s.at[i - 1], az_r.at[i - 1], z_peer[i - 1])

    for i in range(1, nz):
        az_copy(i, False).start()
    for k in range(1, ny):
        by_copy(k, False).start()
    for i in range(1, nz):
        az_copy(i, True).wait_recv()

    def ag_copy(way, part, hop):
        origin = toward(1 - way, hop)
        here = fresh.at[c, origin, rows_of[part]]
        n = ag_slot[way, part, hop]
        return remote(here, here, ag_s.at[n], ag_r.at[n], (y_next, y_prev)[way])

    def ag_arrival(way, part, hop):
        origin = toward(1 - way, hop + 1)
        here = fresh.at[c, origin, rows_of[part]]
        n = ag_slot[way, part, hop]
        return remote(here, here, ag_s.at[n], ag_r.at[n], (y_next, y_prev)[way])

    def ad_copy(n, origin, part, arrival):
        here = fresh.at[1 - c if arrival else c, origin, rows_of[part]]
        return remote(here, here, ad_s.at[n], ad_r.at[n], mate)

    for way, part in even:
        if even[way, part] > 0:
            ag_copy(way, part, 0).start()
    passed = []
    for part in range(2):
        passed.append((y, part))
        ad_copy(len(passed) - 1, y, part, False).start()
    for k in range(1, ny):
        by_copy(k, True).wait_recv()
    for i in range(1, nz):
        bz_copy(i, False).start()
    bd_copy(0, False).start()
    halo_wait(HOPS - 1)
    attend(HOPS, 0, heads)
    for h in range(heads):
        cols = slice(h * HEAD_DIM, (h + 1) * HEAD_DIM)
        att_v[:, cols] = (acc_s[h] / l_s[h]).astype(BF16)
    att_out = pltpu.make_async_copy(att_v, att_h, osem.at[0])
    att_out.start()
    for hop in range(ny // 2):
        for way, part in even:
            if hop >= even[way, part]:
                continue
            ag_arrival(way, part, hop).wait_recv()
            if hop + 1 < even[way, part]:
                ag_copy(way, part, hop + 1).start()
            origin = toward(1 - way, hop + 1)
            passed.append((origin, part))
            ad_copy(len(passed) - 1, origin, part, False).start()
        if hop == ny // 2 - 2:
            for i in range(1, nz):
                bz_copy(i, True).wait_recv()
                bd_copy(i, False).start()
    for i in range(nz):
        bd_copy(i, True).wait_recv()
    for n, (origin, part) in enumerate(passed):
        ad_copy(n, origin, part, True).wait_recv()

    loads[9].wait()
    queries_y, queries_z = fq[:, :ag_lanes], fq[:, ag_lanes:]

    def weights(ref, which):
        return jnp.concatenate(
            [ref[b % 2, b // 2] for b in range(which * nb, (which + 1) * nb)], axis=0
        )

    def project(which):
        return contract_cols(queries_y, weights(fresh, which)) + contract_cols(
            queries_z, weights(fresh_z, which)
        )

    hidden = (jax.nn.silu(project(0)) * project(1)).astype(BF16)
    out_v[:, :ag_lanes] = jnp.dot(hidden, weights(fresh, 2), preferred_element_type=F32).astype(BF16)
    out_v[:, ag_lanes:] = jnp.dot(hidden, weights(fresh_z, 2), preferred_element_type=F32).astype(BF16)
    fast_out = pltpu.make_async_copy(out_v, out_h, osem.at[1])
    fast_out.start()

    for step in range(HOPS):
        halo_send_wait(step)
    for part in range(2):
        pair_copy(part).wait_send()
    term_copy.wait_send()
    for way, part, hop in slot:
        rs_copy(way, part, hop).wait_send()
    for way, part, hop in ag_slot:
        ag_copy(way, part, hop).wait_send()
    for i in range(1, nz):
        zs_copy(i).wait_send()
        az_copy(i, False).wait_send()
        zz_copy(i).wait_send()
        bz_copy(i, False).wait_send()
    for k in range(1, ny):
        zy_copy(k).wait_send()
        by_copy(k, False).wait_send()
    for i in range(nz):
        bd_copy(i, False).wait_send()
    for n, (origin, part) in enumerate(passed):
        ad_copy(n, origin, part, False).wait_send()
    att_out.wait()
    fast_out.wait()


def solution(mesh):
    nz = 4 if mesh.shape["seq"] == 64 else 2
    ny = mesh.shape["seq"] // (2 * nz)

    def body(att_q, att_k, att_v, fast_q, fast_k, fast_v, rates, w_gate, w_up, w_down):
        tok, feat = att_q.shape
        hid = w_gate.shape[1]
        heads = feat // HEAD_DIM
        n_slot = 2 * (ny - 1)
        rs_lanes, ag_lanes = feat - RS_Z, feat - AG_Z
        zrow = BLK // nz
        dma = pltpu.SemaphoreType.DMA
        vmem = pltpu.VMEM
        hbm = pl.BlockSpec(memory_space=pl.ANY)
        return pl.pallas_call(
            functools.partial(kernel, ny, nz, rs_lanes, ag_lanes),
            out_shape=(
                jax.ShapeDtypeStruct((tok, feat), BF16),
                jax.ShapeDtypeStruct((tok, feat), BF16),
            ),
            in_specs=[hbm] * 10,
            out_specs=(hbm, hbm),
            scratch_shapes=[
                vmem((tok, feat), BF16),
                vmem((2, tok, feat), BF16),
                vmem((HOPS, 2, tok, feat), BF16),
                vmem((tok, feat), BF16),
                vmem((2, 2, tok, feat), BF16),
                vmem((1, tok), F32),
                vmem((3, feat, hid), BF16),
                vmem((2, tok, ny * BLK), BF16),
                vmem((tok, ny * BLK), BF16),
                vmem((ny, BLK, rs_lanes), F32),
                vmem((n_slot, BLK // 2, rs_lanes), F32),
                vmem((BLK, rs_lanes), F32),
                vmem((nz - 1, zrow, rs_lanes), F32),
                vmem((BLK, feat), F32),
                vmem((2, ny, BLK, ag_lanes), BF16),
                vmem((ny, BLK, RS_Z), F32),
                vmem((ny, BLK, RS_Z), BF16),
                vmem((nz - 1, ny, zrow, RS_Z), BF16),
                vmem((ny, zrow, RS_Z), F32),
                vmem((ny, zrow, RS_Z), BF16),
                vmem((ny - 1, zrow, RS_Z), BF16),
                vmem((2, ny, BLK, AG_Z), BF16),
                vmem((heads, tok, 1), F32),
                vmem((heads, tok, 1), F32),
                vmem((heads, tok, HEAD_DIM), F32),
                vmem((tok, feat), BF16),
                vmem((tok, feat), BF16),
                dma((10,)),
                dma((2,)),
                dma((HOPS, 2)),
                dma((HOPS, 2)),
                dma((2,)),
                dma((2,)),
                dma,
                dma,
                dma((n_slot,)),
                dma((n_slot,)),
                dma((nz - 1,)),
                dma((nz - 1,)),
                dma((nz - 1,)),
                dma((nz - 1,)),
                dma((n_slot,)),
                dma((n_slot,)),
                dma((2 * ny,)),
                dma((2 * ny,)),
                dma((nz - 1,)),
                dma((nz - 1,)),
                dma((ny - 1,)),
                dma((ny - 1,)),
                dma((ny - 1,)),
                dma((ny - 1,)),
                dma((nz - 1,)),
                dma((nz - 1,)),
                dma((nz,)),
                dma((nz,)),
            ],
            compiler_params=pltpu.CompilerParams(
                collective_id=0, has_side_effects=True, vmem_limit_bytes=60 * 1024 * 1024
            ),
        )(
            att_q, att_k, att_v, fast_q, fast_k, fast_v, rates.reshape(1, -1),
            w_gate, w_up, w_down,
        )

    rows = P("seq", "head")
    weights = P(None, "head")
    return jax.shard_map(
        body,
        mesh=mesh,
        in_specs=(rows,) * 6 + (P("seq"),) + (weights,) * 3,
        out_specs=(rows, rows),
        check_vma=False,
    )
```

```python
import functools

import jax
import jax.numpy as jnp
from jax import lax
from jax.experimental import pallas as pl
from jax.experimental.pallas import tpu as pltpu
from jax.sharding import PartitionSpec as P

HEAD_DIM = 128
BLK = 128
HOPS = 4
RS_Z = 256
AG_Z = 128
NORM_EPS = 1e-06
MASKED = -1e30
MESH = pl.DeviceIdType.MESH
F32 = jnp.float32
BF16 = jnp.bfloat16


def silu_parts(pre_act):
    sig = jax.nn.sigmoid(pre_act)
    return pre_act * sig, sig * (1.0 + pre_act * (1.0 - sig))


def contract_rows(lhs, rhs):
    return lax.dot_general(lhs, rhs, (((0,), (0,)), ((), ())), preferred_element_type=F32)


def contract_cols(lhs, rhs):
    return lax.dot_general(lhs, rhs, (((1,), (1,)), ((), ())), preferred_element_type=F32)


def kernel(
    ny, nz, rs_lanes, ag_lanes,
    aq_h, ak_h, av_h, fq_h, fk_h, fv_h, lr_h, wg_h, wu_h, wd_h,
    att_h, out_h,
    aq, okv, halo, fq, kvf, lr, w3, tt, rt, grad, ry, zs, zr, old_t, fresh,
    g_z, gb_z, in_z, q_z, qb_z, in_y, fresh_z,
    m_s, l_s, acc_s, att_v, out_v,
    loc, osem, hs, hr, ps, pr, ts, tr, rs_s, rs_r, zs_s, zs_r, az_s, az_r, ag_s, ag_r, ad_s, ad_r,
    zz_s, zz_r, zy_s, zy_r, by_s, by_r, bz_s, bz_r, bd_s, bd_r,
):
    tok, feat = aq.shape
    nb = w3.shape[2] // BLK
    heads = feat // HEAD_DIM
    half = BLK // 2
    zrow = BLK // nz
    s = lax.axis_index("seq")
    total = 2 * ny * nz
    c = lax.rem(s, 2)
    y = lax.rem(s // 2, ny)
    z = s // (2 * ny)
    mate = s + 1 - 2 * c
    y_next = z * 2 * ny + lax.rem(y + 1, ny) * 2 + c
    y_prev = z * 2 * ny + lax.rem(y + ny - 1, ny) * 2 + c
    y_peer = [z * 2 * ny + lax.rem(y + k, ny) * 2 + c for k in range(1, ny)]
    z_peer = [lax.rem(z + i, nz) * 2 * ny + y * 2 + c for i in range(1, nz)]
    chain = {(1, 0): ny // 2, (1, 1): ny // 2, (0, 0): ny // 2 - 1, (0, 1): ny // 2 - 1}
    even = chain

    def remote(src, dst, ssem, rsem, dev):
        return pltpu.make_async_remote_copy(
            src_ref=src, dst_ref=dst, send_sem=ssem, recv_sem=rsem,
            device_id={"seq": dev}, device_id_type=MESH,
        )

    loads = [
        (fk_h, kvf.at[0, 0]), (wg_h, w3.at[0]), (wu_h, w3.at[1]), (lr_h, lr),
        (fv_h, kvf.at[0, 1]), (wd_h, w3.at[2]),
        (aq_h, aq), (ak_h, okv.at[0]), (av_h, okv.at[1]), (fq_h, fq),
    ]
    loads = [pltpu.make_async_copy(src, dst, loc.at[i]) for i, (src, dst) in enumerate(loads)]
    for one in loads:
        one.start()

    barrier = pltpu.get_barrier_semaphore()
    for peer in [mate] + y_peer + z_peer:
        pl.semaphore_signal(barrier, inc=1, device_id={"seq": peer}, device_id_type=MESH)

    @pl.when((c == 1) & (s < total - 1))
    def _():
        pl.semaphore_signal(barrier, inc=1, device_id={"seq": s + 1}, device_id_type=MESH)

    @pl.when((c == 0) & (s > 0))
    def _():
        pl.semaphore_signal(barrier, inc=1, device_id={"seq": s - 1}, device_id_type=MESH)

    beside = c * (1 - s // (total - 1)) + (1 - c) * ((s + total - 1) // total)

    def halo_copy(step, part, dev):
        if step == 0:
            src = (ak_h, av_h)[part]
        else:
            src = halo.at[step - 1, part]
        return remote(src, halo.at[step, part], hs.at[step, part], hr.at[step, part], dev)

    def halo_send(step):
        @pl.when((s < total - 1) & (s >= step))
        def _():
            for part in range(2):
                halo_copy(step, part, s + 1).start()

    def halo_send_wait(step):
        @pl.when((s < total - 1) & (s >= step))
        def _():
            for part in range(2):
                halo_copy(step, part, s + 1).wait_send()

    def halo_wait(step):
        @pl.when(s >= step + 1)
        def _():
            for part in range(2):
                halo_copy(step, part, s - 1).wait_recv()

    def pair_copy(part):
        return remote((fk_h, fv_h)[part], kvf.at[1, part], ps.at[part], pr.at[part], mate)

    edge = 2 * y + c == 2 * ny - 1

    def halo_turn(step, core, at_edge=None):
        due = c == core
        if at_edge is not None:
            due = edge if at_edge else due & jnp.logical_not(edge)

        @pl.when(due)
        def _():
            halo_wait(step - 1)
            halo_send(step)

    scale = HEAD_DIM ** (-0.5)

    def attend(delta, lo, hi):
        def one_head(h, _):
            cols = pl.ds(pl.multiple_of(h * HEAD_DIM, HEAD_DIM), HEAD_DIM)
            kv = okv if delta == 0 else halo.at[delta - 1]
            key, val = kv[0, :, cols], kv[1, :, cols]
            sc = contract_cols(aq[:, cols], key) * scale
            if delta in (0, HOPS):
                qi = lax.broadcasted_iota(jnp.int32, (tok, tok), 0)
                ki = lax.broadcasted_iota(jnp.int32, (tok, tok), 1)
                keep = (ki <= qi) if delta == 0 else (ki > qi)
                sc = jnp.where(keep, sc, MASKED)
            top = jnp.max(sc, axis=1, keepdims=True)
            if delta == 0:
                p = jnp.exp(sc - top)
                m_s[h] = top
                l_s[h] = jnp.sum(p, axis=1, keepdims=True)
                acc_s[h] = jnp.dot(p.astype(BF16), val, preferred_element_type=F32)
            else:
                m_old = m_s[h]
                m_new = jnp.maximum(m_old, top)
                p = jnp.exp(sc - m_new)
                alpha = jnp.exp(m_old - m_new)
                m_s[h] = m_new
                l_s[h] = l_s[h] * alpha + jnp.sum(p, axis=1, keepdims=True)
                acc_s[h] = acc_s[h] * alpha + jnp.dot(p.astype(BF16), val, preferred_element_type=F32)
            return 0

        if delta == 0:
            lax.fori_loop(lo, hi, one_head, 0)
        else:
            @pl.when(s >= delta)
            def _():
                lax.fori_loop(lo, hi, one_head, 0)

    loads[0].wait()
    loads[1].wait()
    loads[2].wait()
    loads[3].wait()
    keys = kvf[0, 0]
    eye = lax.broadcasted_iota(jnp.int32, (tok, tok), 0) == lax.broadcasted_iota(jnp.int32, (tok, tok), 1)
    rate = jnp.sum(jnp.where(eye, jnp.broadcast_to(lr[...], (tok, tok)), 0.0), axis=1, keepdims=True)
    if 2 * ny > 3 * nb:
        for b in range(3 * nb, 2 * ny):
            tt[b % 2, :, (b // 2) * BLK:(b // 2 + 1) * BLK] = jnp.zeros((tok, BLK), BF16)

    def put(b, value):
        tt[b % 2, :, (b // 2) * BLK:(b // 2 + 1) * BLK] = value.astype(BF16)

    pre_gate = jnp.dot(keys, w3[0], preferred_element_type=F32)
    pre_up = jnp.dot(keys, w3[1], preferred_element_type=F32)
    loads[4].wait()
    loads[5].wait()
    back = jnp.dot(kvf[0, 1], w3[2], preferred_element_type=F32)
    for i in range(nb):
        cols = slice(i * BLK, (i + 1) * BLK)
        pg, pu, bk = pre_gate[:, cols], pre_up[:, cols], back[:, cols]
        silu, slope = silu_parts(pg)
        rb = rate * bk
        put(i, rb * pu * slope)
        put(nb + i, rb * silu)
        put(2 * nb + i, rate * silu * pu)
    pl.semaphore_wait(barrier, 1 + len(y_peer) + len(z_peer) + beside)
    for part in range(2):
        pair_copy(part).start()
    term_copy = remote(tt.at[1 - c], rt, ts, tr, mate)
    term_copy.start()
    halo_send(0)

    split = nb * BLK
    width = ny * BLK
    lanes_y, lanes_z = pl.ds(0, rs_lanes), pl.ds(rs_lanes, feat - rs_lanes)

    def add_grads(terms, side, lanes, into, first):
        low = contract_rows(terms(0, split), kvf[side, 0, :, lanes]).reshape(nb, BLK, -1)
        high = contract_rows(terms(split, width), kvf[side, 1, :, lanes]).reshape(ny - nb, BLK, -1)
        if first:
            into[0:nb], into[nb:ny] = low, high
        else:
            into[0:nb] += low
            into[nb:ny] += high

    def own_terms(lo, hi):
        return tt[c, :, lo:hi]

    def mate_terms(lo, hi):
        return rt[:, lo:hi]

    add_grads(own_terms, 0, lanes_z, g_z, True)
    add_grads(own_terms, 0, lanes_y, grad, True)
    for i in range(6, 9):
        loads[i].wait()
    attend(0, 0, 1)
    term_copy.wait_recv()
    for part in range(2):
        pair_copy(part).wait_recv()
    add_grads(mate_terms, 1, lanes_z, g_z, False)

    def z_rows(i):
        return pl.ds(pl.multiple_of(lax.rem(z + i, nz) * zrow, zrow), zrow)

    gb_z[...] = g_z[...].astype(BF16)

    def zz_copy(i):
        return remote(gb_z.at[:, z_rows(i)], in_z.at[i - 1], zz_s.at[i - 1], zz_r.at[i - 1], z_peer[i - 1])

    def zy_copy(k):
        return remote(
            qb_z.at[lax.rem(y + k, ny)], in_y.at[k - 1], zy_s.at[k - 1], zy_r.at[k - 1], y_peer[k - 1]
        )

    for i in range(1, nz):
        zz_copy(i).start()
    add_grads(mate_terms, 1, lanes_y, grad, False)

    def turn_z():
        got = g_z[:, z_rows(0), :]
        for i in range(1, nz):
            zz_copy(i).wait_recv()
            got += in_z[i - 1].astype(F32)
        q_z[...] = got
        qb_z[...] = got.astype(BF16)
        for k in range(1, ny):
            zy_copy(k).start()

    rows_of = [pl.ds(0, half), pl.ds(half, half)]
    slot, ag_slot = {}, {}
    for way in range(2):
        for part in range(2):
            for hop in range(chain[way, part]):
                slot[way, part, hop] = len(slot)
            for hop in range(even[way, part]):
                ag_slot[way, part, hop] = len(ag_slot)

    def toward(way, dist):
        return lax.rem(y + dist, ny) if way == 0 else lax.rem(y + ny - dist, ny)

    def rs_copy(way, part, hop):
        if hop == 0:
            src = grad.at[toward(way, chain[way, part]), rows_of[part]]
        else:
            src = ry.at[slot[way, part, hop - 1]]
        n = slot[way, part, hop]
        return remote(src, ry.at[n], rs_s.at[n], rs_r.at[n], (y_next, y_prev)[way])

    for way, part in chain:
        rs_copy(way, part, 0).start()
    attend(0, 1, 3)

    def rs_step(way, hop):
        for part in range(2):
            rs_copy(way, part, hop).wait_recv()
            if hop + 1 < chain[way, part]:
                n = slot[way, part, hop]
                ry[n] += grad[toward(way, chain[way, part] - hop - 1), rows_of[part]]
                rs_copy(way, part, hop + 1).start()

    rs_step(1, 0)
    attend(0, 3, heads)
    rs_step(0, 0)
    rs_step(1, 1)
    halo_wait(0)

    @pl.when(c == 0)
    def _():
        halo_send(1)

    rs_step(0, 1)
    attend(1, 0, 2)
    rs_step(1, 2)
    turn_z()

    @pl.when(c == 1)
    def _():
        halo_send(1)

    rs_step(0, 2)
    rs_step(1, 3)
    for part in range(2):
        got = grad[y, rows_of[part]]
        for way in range(2):
            if chain[way, part] > 0:
                got += ry[slot[way, part, chain[way, part] - 1]]
        zs[rows_of[part]] = got

    def zs_copy(i):
        return remote(zs.at[z_rows(i)], zr.at[i - 1], zs_s.at[i - 1], zs_r.at[i - 1], z_peer[i - 1])

    for i in range(1, nz):
        zs_copy(i).start()
    own_b = 2 * y + c
    src_b = jnp.minimum(own_b, 3 * nb - 1)
    old_cols = pl.ds(pl.multiple_of(lax.rem(src_b, nb) * BLK, BLK), BLK)
    old_t[...] = w3[src_b // nb, :, old_cols].astype(F32).T
    old = old_t[z_rows(0), :]
    old_norm = jnp.sqrt(jnp.sum(old * old, axis=1, keepdims=True))
    halo_turn(2, 1, False)
    attend(1, 2, heads)
    sum_z = q_z[y]
    for k in range(1, ny):
        zy_copy(k).wait_recv()
        sum_z += in_y[k - 1].astype(F32)
    sum_y = zs[z_rows(0), :]
    for i in range(1, nz):
        zs_copy(i).wait_recv()
        sum_y += zr[i - 1]
    updated = old + jnp.concatenate([sum_y, sum_z], axis=1)
    squares = jnp.sum(updated * updated, axis=1, keepdims=True)
    new = (updated * (old_norm / jnp.sqrt(squares + NORM_EPS))).astype(BF16)
    fresh[c, y, z_rows(0), :] = new[:, :ag_lanes]
    fresh_z[c, y, z_rows(0), :] = new[:, ag_lanes:]

    def by_copy(k, arrival):
        here = fresh_z.at[c, lax.rem(y + ny - k, ny) if arrival else y, z_rows(0)]
        return remote(here, here, by_s.at[k - 1], by_r.at[k - 1], y_peer[k - 1])

    def bz_copy(i, arrival):
        here = fresh_z.at[c, :, z_rows(nz - i) if arrival else z_rows(0)]
        return remote(here, here, bz_s.at[i - 1], bz_r.at[i - 1], z_peer[i - 1])

    def bd_copy(i, arrival):
        here = fresh_z.at[1 - c if arrival else c, :, z_rows(nz - i)]
        return remote(here, here, bd_s.at[i], bd_r.at[i], mate)

    def az_copy(i, arrival):
        here = fresh.at[c, y, z_rows(nz - i) if arrival else z_rows(0)]
        return remote(here, here, az_s.at[i - 1], az_r.at[i - 1], z_peer[i - 1])

    for i in range(1, nz):
        az_copy(i, False).start()
    for k in range(1, ny):
        by_copy(k, False).start()
    halo_turn(2, 1, True)
    halo_turn(2, 0)
    attend(2, 0, 3)
    for i in range(1, nz):
        az_copy(i, True).wait_recv()

    def ag_copy(way, part, hop):
        origin = toward(1 - way, hop)
        here = fresh.at[c, origin, rows_of[part]]
        n = ag_slot[way, part, hop]
        return remote(here, here, ag_s.at[n], ag_r.at[n], (y_next, y_prev)[way])

    def ag_arrival(way, part, hop):
        origin = toward(1 - way, hop + 1)
        here = fresh.at[c, origin, rows_of[part]]
        n = ag_slot[way, part, hop]
        return remote(here, here, ag_s.at[n], ag_r.at[n], (y_next, y_prev)[way])

    def ad_copy(n, origin, part, arrival):
        here = fresh.at[1 - c if arrival else c, origin, rows_of[part]]
        return remote(here, here, ad_s.at[n], ad_r.at[n], mate)

    for way, part in even:
        if even[way, part] > 0:
            ag_copy(way, part, 0).start()
    passed = []
    for part in range(2):
        passed.append((y, part))
        ad_copy(len(passed) - 1, y, part, False).start()
    attend(2, 3, heads)
    for hop in range(ny // 2):
        for way, part in even:
            if hop >= even[way, part]:
                continue
            ag_arrival(way, part, hop).wait_recv()
            if hop + 1 < even[way, part]:
                ag_copy(way, part, hop + 1).start()
            origin = toward(1 - way, hop + 1)
            passed.append((origin, part))
            ad_copy(len(passed) - 1, origin, part, False).start()
        if hop == ny // 2 - 2:
            for i in range(1, nz):
                bz_copy(i, True).wait_recv()
                bd_copy(i, False).start()
        if hop == 0:
            for k in range(1, ny):
                by_copy(k, True).wait_recv()
            for i in range(1, nz):
                bz_copy(i, False).start()
            bd_copy(0, False).start()
        if hop == 1:
            halo_turn(3, 1)
            halo_turn(3, 0)
            attend(3, 0, 3)
        if hop == 2:
            attend(3, 3, heads)
    halo_wait(HOPS - 1)
    attend(HOPS, 0, heads)
    for h in range(heads):
        cols = slice(h * HEAD_DIM, (h + 1) * HEAD_DIM)
        att_v[:, cols] = (acc_s[h] / l_s[h]).astype(BF16)
    att_out = pltpu.make_async_copy(att_v, att_h, osem.at[0])
    att_out.start()
    for i in range(nz):
        bd_copy(i, True).wait_recv()
    for n, (origin, part) in enumerate(passed):
        ad_copy(n, origin, part, True).wait_recv()

    loads[9].wait()
    queries_y, queries_z = fq[:, :ag_lanes], fq[:, ag_lanes:]

    def weights(ref, which):
        return jnp.concatenate(
            [ref[b % 2, b // 2] for b in range(which * nb, (which + 1) * nb)], axis=0
        )

    def project(which):
        return contract_cols(queries_y, weights(fresh, which)) + contract_cols(
            queries_z, weights(fresh_z, which)
        )

    hidden = (jax.nn.silu(project(0)) * project(1)).astype(BF16)
    out_v[:, :ag_lanes] = jnp.dot(hidden, weights(fresh, 2), preferred_element_type=F32).astype(BF16)
    out_v[:, ag_lanes:] = jnp.dot(hidden, weights(fresh_z, 2), preferred_element_type=F32).astype(BF16)
    fast_out = pltpu.make_async_copy(out_v, out_h, osem.at[1])
    fast_out.start()

    for step in range(HOPS):
        halo_send_wait(step)
    for part in range(2):
        pair_copy(part).wait_send()
    term_copy.wait_send()
    for way, part, hop in slot:
        rs_copy(way, part, hop).wait_send()
    for way, part, hop in ag_slot:
        ag_copy(way, part, hop).wait_send()
    for i in range(1, nz):
        zs_copy(i).wait_send()
        az_copy(i, False).wait_send()
        zz_copy(i).wait_send()
        bz_copy(i, False).wait_send()
    for k in range(1, ny):
        zy_copy(k).wait_send()
        by_copy(k, False).wait_send()
    for i in range(nz):
        bd_copy(i, False).wait_send()
    for n, (origin, part) in enumerate(passed):
        ad_copy(n, origin, part, False).wait_send()
    att_out.wait()
    fast_out.wait()


def solution(mesh):
    nz = 4 if mesh.shape["seq"] == 64 else 2
    ny = mesh.shape["seq"] // (2 * nz)

    def body(att_q, att_k, att_v, fast_q, fast_k, fast_v, rates, w_gate, w_up, w_down):
        tok, feat = att_q.shape
        hid = w_gate.shape[1]
        heads = feat // HEAD_DIM
        n_slot = 2 * (ny - 1)
        rs_lanes, ag_lanes = feat - RS_Z, feat - AG_Z
        zrow = BLK // nz
        dma = pltpu.SemaphoreType.DMA
        vmem = pltpu.VMEM
        hbm = pl.BlockSpec(memory_space=pl.ANY)
        return pl.pallas_call(
            functools.partial(kernel, ny, nz, rs_lanes, ag_lanes),
            out_shape=(
                jax.ShapeDtypeStruct((tok, feat), BF16),
                jax.ShapeDtypeStruct((tok, feat), BF16),
            ),
            in_specs=[hbm] * 10,
            out_specs=(hbm, hbm),
            scratch_shapes=[
                vmem((tok, feat), BF16),
                vmem((2, tok, feat), BF16),
                vmem((HOPS, 2, tok, feat), BF16),
                vmem((tok, feat), BF16),
                vmem((2, 2, tok, feat), BF16),
                vmem((1, tok), F32),
                vmem((3, feat, hid), BF16),
                vmem((2, tok, ny * BLK), BF16),
                vmem((tok, ny * BLK), BF16),
                vmem((ny, BLK, rs_lanes), F32),
                vmem((n_slot, BLK // 2, rs_lanes), F32),
                vmem((BLK, rs_lanes), F32),
                vmem((nz - 1, zrow, rs_lanes), F32),
                vmem((BLK, feat), F32),
                vmem((2, ny, BLK, ag_lanes), BF16),
                vmem((ny, BLK, RS_Z), F32),
                vmem((ny, BLK, RS_Z), BF16),
                vmem((nz - 1, ny, zrow, RS_Z), BF16),
                vmem((ny, zrow, RS_Z), F32),
                vmem((ny, zrow, RS_Z), BF16),
                vmem((ny - 1, zrow, RS_Z), BF16),
                vmem((2, ny, BLK, AG_Z), BF16),
                vmem((heads, tok, 1), F32),
                vmem((heads, tok, 1), F32),
                vmem((heads, tok, HEAD_DIM), F32),
                vmem((tok, feat), BF16),
                vmem((tok, feat), BF16),
                dma((10,)),
                dma((2,)),
                dma((HOPS, 2)),
                dma((HOPS, 2)),
                dma((2,)),
                dma((2,)),
                dma,
                dma,
                dma((n_slot,)),
                dma((n_slot,)),
                dma((nz - 1,)),
                dma((nz - 1,)),
                dma((nz - 1,)),
                dma((nz - 1,)),
                dma((n_slot,)),
                dma((n_slot,)),
                dma((2 * ny,)),
                dma((2 * ny,)),
                dma((nz - 1,)),
                dma((nz - 1,)),
                dma((ny - 1,)),
                dma((ny - 1,)),
                dma((ny - 1,)),
                dma((ny - 1,)),
                dma((nz - 1,)),
                dma((nz - 1,)),
                dma((nz,)),
                dma((nz,)),
            ],
            compiler_params=pltpu.CompilerParams(
                collective_id=0, has_side_effects=True, vmem_limit_bytes=60 * 1024 * 1024
            ),
        )(
            att_q, att_k, att_v, fast_q, fast_k, fast_v, rates.reshape(1, -1),
            w_gate, w_up, w_down,
        )

    rows = P("seq", "head")
    weights = P(None, "head")
    return jax.shard_map(
        body,
        mesh=mesh,
        in_specs=(rows,) * 6 + (P("seq"),) + (weights,) * 3,
        out_specs=(rows, rows),
        check_vma=False,
    )
```

```python
import functools

import jax
import jax.numpy as jnp
from jax import lax
from jax.experimental import pallas as pl
from jax.experimental.pallas import tpu as pltpu
from jax.sharding import PartitionSpec as P

HEAD_DIM = 128
BLK = 128
HOPS = 4
RS_Z = 256
AG_Z = 128
NORM_EPS = 1e-06
LOG2_E = 1.4426950408889634
MASKED = -1e30
MESH = pl.DeviceIdType.MESH
F32 = jnp.float32
BF16 = jnp.bfloat16


def silu_parts(pre_act):
    sig = jax.nn.sigmoid(pre_act)
    return pre_act * sig, sig * (1.0 + pre_act * (1.0 - sig))


def contract_rows(lhs, rhs):
    return lax.dot_general(lhs, rhs, (((0,), (0,)), ((), ())), preferred_element_type=F32)


def contract_cols(lhs, rhs):
    return lax.dot_general(lhs, rhs, (((1,), (1,)), ((), ())), preferred_element_type=F32)


def kernel(
    ny, nz, rs_lanes, ag_lanes,
    aq_h, ak_h, av_h, fq_h, fk_h, fv_h, lr_h, wg_h, wu_h, wd_h,
    att_v, out_v,
    aq, okv, halo, fq, kvf, lr, w3, tt, rt, grad, ry, zs, zr, old_t, fresh,
    g_z, gb_z, in_z, q_z, qb_z, in_y, fresh_z,
    m_s, l_s, acc_s,
    loc, hs, hr, ps, pr, ts, tr, rs_s, rs_r, zs_s, zs_r, az_s, az_r, ag_s, ag_r, ad_s, ad_r,
    zz_s, zz_r, zy_s, zy_r, by_s, by_r, bz_s, bz_r, bd_s, bd_r,
):
    tok, feat = aq.shape
    nb = w3.shape[2] // BLK
    heads = feat // HEAD_DIM
    half = BLK // 2
    zrow = BLK // nz
    s = lax.axis_index("seq")
    total = 2 * ny * nz
    c = lax.rem(s, 2)
    y = lax.rem(s // 2, ny)
    z = s // (2 * ny)
    mate = s + 1 - 2 * c
    y_next = z * 2 * ny + lax.rem(y + 1, ny) * 2 + c
    y_prev = z * 2 * ny + lax.rem(y + ny - 1, ny) * 2 + c
    y_peer = [z * 2 * ny + lax.rem(y + k, ny) * 2 + c for k in range(1, ny)]
    z_peer = [lax.rem(z + i, nz) * 2 * ny + y * 2 + c for i in range(1, nz)]
    chain = {(1, 0): ny // 2, (1, 1): ny // 2, (0, 0): ny // 2 - 1, (0, 1): ny // 2 - 1}
    even = chain

    def remote(src, dst, ssem, rsem, dev):
        return pltpu.make_async_remote_copy(
            src_ref=src, dst_ref=dst, send_sem=ssem, recv_sem=rsem,
            device_id={"seq": dev}, device_id_type=MESH,
        )

    loads = [
        (fk_h, kvf.at[0, 0]), (wg_h, w3.at[0]), (wu_h, w3.at[1]), (lr_h, lr),
        (fv_h, kvf.at[0, 1]), (wd_h, w3.at[2]),
        (aq_h, aq), (ak_h, okv.at[0]), (av_h, okv.at[1]), (fq_h, fq),
    ]
    loads = [pltpu.make_async_copy(src, dst, loc.at[i]) for i, (src, dst) in enumerate(loads)]
    for one in loads:
        one.start()

    barrier = pltpu.get_barrier_semaphore()
    for peer in [mate] + y_peer + z_peer:
        pl.semaphore_signal(barrier, inc=1, device_id={"seq": peer}, device_id_type=MESH)

    @pl.when((c == 1) & (s < total - 1))
    def _():
        pl.semaphore_signal(barrier, inc=1, device_id={"seq": s + 1}, device_id_type=MESH)

    @pl.when((c == 0) & (s > 0))
    def _():
        pl.semaphore_signal(barrier, inc=1, device_id={"seq": s - 1}, device_id_type=MESH)

    @pl.when((c == 0) & (y == 0) & (z > 0))
    def _():
        pl.semaphore_signal(barrier, inc=1, device_id={"seq": s - 2}, device_id_type=MESH)

    beside = (1 - c) * (y // (ny - 1)) * (1 - z // (nz - 1)) + c * (1 - s // (total - 1)) + (1 - c) * ((s + total - 1) // total)

    place = 2 * y + c
    edge = place == 2 * ny - 1
    straight = (place == 2 * ny - 2) & (z < nz - 1)

    def straight_copy(part):
        return remote((ak_h, av_h)[part], halo.at[1, part], hs.at[HOPS, part], hr.at[1, part], s + 2)

    def halo_copy(step, part, dev):
        if step == 0:
            src = (ak_h, av_h)[part]
        else:
            src = halo.at[step - 1, part]
        return remote(src, halo.at[step, part], hs.at[step, part], hr.at[step, part], dev)

    def sends(step):
        due = (s < total - 1) & (s >= step)
        return due & jnp.logical_not(edge) if step == 1 else due

    def halo_send(step):
        @pl.when(sends(step))
        def _():
            for part in range(2):
                halo_copy(step, part, s + 1).start()

    def halo_send_wait(step):
        @pl.when(sends(step))
        def _():
            for part in range(2):
                halo_copy(step, part, s + 1).wait_send()

    def halo_wait(step):
        @pl.when(s >= step + 1)
        def _():
            for part in range(2):
                halo_copy(step, part, s - 1).wait_recv()

    def pair_copy(part):
        return remote((fk_h, fv_h)[part], kvf.at[1, part], ps.at[part], pr.at[part], mate)

    def halo_turn(step, core, at_edge=None):
        due = c == core
        if at_edge is not None:
            due = edge if at_edge else due & jnp.logical_not(edge)

        @pl.when(due)
        def _():
            halo_wait(step - 1)
            halo_send(step)

    scale = HEAD_DIM ** (-0.5) * LOG2_E

    def alone(fn):
        pl.when(s >= 0)(fn)

    def attend(delta, lo, hi):
        def one_head(h):
            cols = slice(h * HEAD_DIM, (h + 1) * HEAD_DIM)
            kv = okv if delta == 0 else halo.at[delta - 1]
            key, val = kv[0, :, cols], kv[1, :, cols]
            sc = contract_cols(aq[:, cols], key)
            if delta in (0, HOPS):
                qi = lax.broadcasted_iota(jnp.int32, (tok, tok), 0)
                ki = lax.broadcasted_iota(jnp.int32, (tok, tok), 1)
                keep = (ki <= qi) if delta == 0 else (ki > qi)
                sc = jnp.where(keep, sc, MASKED)
            top = jnp.max(sc, axis=1, keepdims=True)
            if delta == 0:
                p = jnp.exp2((sc - top) * scale)
                m_s[h] = top
                l_s[h] = jnp.sum(p, axis=1, keepdims=True)
                acc_s[h] = jnp.dot(p.astype(BF16), val, preferred_element_type=F32)
            else:
                m_old = m_s[h]
                m_new = jnp.maximum(m_old, top)
                p = jnp.exp2((sc - m_new) * scale)
                alpha = jnp.exp2((m_old - m_new) * scale)
                m_s[h] = m_new
                l_s[h] = l_s[h] * alpha + jnp.sum(p, axis=1, keepdims=True)
                acc_s[h] = acc_s[h] * alpha + jnp.dot(p.astype(BF16), val, preferred_element_type=F32)

        if delta == 0:
            @alone
            def _():
                for h in range(lo, hi):
                    one_head(h)
        else:
            @pl.when(s >= delta)
            def _():
                for h in range(lo, hi):
                    one_head(h)

    loads[0].wait()
    loads[1].wait()
    loads[2].wait()
    loads[3].wait()
    keys = kvf[0, 0]
    eye = lax.broadcasted_iota(jnp.int32, (tok, tok), 0) == lax.broadcasted_iota(jnp.int32, (tok, tok), 1)
    rate = jnp.sum(jnp.where(eye, jnp.broadcast_to(lr[...], (tok, tok)), 0.0), axis=1, keepdims=True)
    if 2 * ny > 3 * nb:
        for b in range(3 * nb, 2 * ny):
            tt[b % 2, :, (b // 2) * BLK:(b // 2 + 1) * BLK] = jnp.zeros((tok, BLK), BF16)

    def put(b, value):
        tt[b % 2, :, (b // 2) * BLK:(b // 2 + 1) * BLK] = value.astype(BF16)

    pre_gate = jnp.dot(keys, w3[0], preferred_element_type=F32)
    pre_up = jnp.dot(keys, w3[1], preferred_element_type=F32)
    loads[4].wait()
    loads[5].wait()
    back = jnp.dot(kvf[0, 1], w3[2], preferred_element_type=F32)
    for i in range(nb):
        cols = slice(i * BLK, (i + 1) * BLK)
        pg, pu, bk = pre_gate[:, cols], pre_up[:, cols], back[:, cols]
        silu, slope = silu_parts(pg)
        rb = rate * bk
        put(i, rb * pu * slope)
        put(nb + i, rb * silu)
        put(2 * nb + i, rate * silu * pu)
    pl.semaphore_wait(barrier, 1 + len(y_peer) + len(z_peer) + beside)
    for part in range(2):
        pair_copy(part).start()
    term_copy = remote(tt.at[1 - c], rt, ts, tr, mate)
    term_copy.start()
    halo_send(0)

    @pl.when(straight)
    def _():
        for part in range(2):
            straight_copy(part).start()


    split = nb * BLK
    width = ny * BLK
    lanes_y, lanes_z = pl.ds(0, rs_lanes), pl.ds(rs_lanes, feat - rs_lanes)

    def add_grads(terms, side, lanes, into, first):
        low = contract_rows(terms(0, split), kvf[side, 0, :, lanes]).reshape(nb, BLK, -1)
        high = contract_rows(terms(split, width), kvf[side, 1, :, lanes]).reshape(ny - nb, BLK, -1)
        if first:
            into[0:nb], into[nb:ny] = low, high
        else:
            into[0:nb] += low
            into[nb:ny] += high

    def own_terms(lo, hi):
        return tt[c, :, lo:hi]

    def mate_terms(lo, hi):
        return rt[:, lo:hi]

    @alone
    def _():
        add_grads(own_terms, 0, lanes_z, g_z, True)
        add_grads(own_terms, 0, lanes_y, grad, True)

    for i in range(6, 9):
        loads[i].wait()
    attend(0, 0, 1)
    term_copy.wait_recv()
    for part in range(2):
        pair_copy(part).wait_recv()
    @alone
    def _():
        add_grads(mate_terms, 1, lanes_z, g_z, False)


    def z_rows(i):
        return pl.ds(pl.multiple_of(lax.rem(z + i, nz) * zrow, zrow), zrow)

    gb_z[...] = g_z[...].astype(BF16)

    def zz_copy(i):
        return remote(gb_z.at[:, z_rows(i)], in_z.at[i - 1], zz_s.at[i - 1], zz_r.at[i - 1], z_peer[i - 1])

    def zy_copy(k):
        return remote(
            qb_z.at[lax.rem(y + k, ny)], in_y.at[k - 1], zy_s.at[k - 1], zy_r.at[k - 1], y_peer[k - 1]
        )

    for i in range(1, nz):
        zz_copy(i).start()
    @alone
    def _():
        add_grads(mate_terms, 1, lanes_y, grad, False)


    def turn_z():
        got = g_z[:, z_rows(0), :]
        for i in range(1, nz):
            zz_copy(i).wait_recv()
            got += in_z[i - 1].astype(F32)
        q_z[...] = got
        qb_z[...] = got.astype(BF16)
        for k in range(1, ny):
            zy_copy(k).start()

    rows_of = [pl.ds(0, half), pl.ds(half, half)]
    slot, ag_slot = {}, {}
    for way in range(2):
        for part in range(2):
            for hop in range(chain[way, part]):
                slot[way, part, hop] = len(slot)
            for hop in range(even[way, part]):
                ag_slot[way, part, hop] = len(ag_slot)

    def toward(way, dist):
        return lax.rem(y + dist, ny) if way == 0 else lax.rem(y + ny - dist, ny)

    def rs_copy(way, part, hop):
        if hop == 0:
            src = grad.at[toward(way, chain[way, part]), rows_of[part]]
        else:
            src = ry.at[slot[way, part, hop - 1]]
        n = slot[way, part, hop]
        return remote(src, ry.at[n], rs_s.at[n], rs_r.at[n], (y_next, y_prev)[way])

    for way, part in chain:
        rs_copy(way, part, 0).start()
    attend(0, 1, 3)

    def rs_step(way, hop):
        for part in range(2):
            rs_copy(way, part, hop).wait_recv()
            if hop + 1 < chain[way, part]:
                n = slot[way, part, hop]
                ry[n] += grad[toward(way, chain[way, part] - hop - 1), rows_of[part]]
                rs_copy(way, part, hop + 1).start()

    rs_step(1, 0)
    attend(0, 3, heads)
    rs_step(0, 0)
    rs_step(1, 1)
    halo_wait(0)

    @pl.when(c == 0)
    def _():
        halo_send(1)

    rs_step(0, 1)
    attend(1, 0, 2)
    rs_step(1, 2)
    turn_z()

    @pl.when(c == 1)
    def _():
        halo_send(1)

    rs_step(0, 2)
    rs_step(1, 3)
    for part in range(2):
        got = grad[y, rows_of[part]]
        for way in range(2):
            if chain[way, part] > 0:
                got += ry[slot[way, part, chain[way, part] - 1]]
        zs[rows_of[part]] = got

    def zs_copy(i):
        return remote(zs.at[z_rows(i)], zr.at[i - 1], zs_s.at[i - 1], zs_r.at[i - 1], z_peer[i - 1])

    for i in range(1, nz):
        zs_copy(i).start()
    own_b = 2 * y + c
    src_b = jnp.minimum(own_b, 3 * nb - 1)
    old_cols = pl.ds(pl.multiple_of(lax.rem(src_b, nb) * BLK, BLK), BLK)
    old_t[...] = w3[src_b // nb, :, old_cols].astype(F32).T
    old = old_t[z_rows(0), :]
    old_norm = jnp.sqrt(jnp.sum(old * old, axis=1, keepdims=True))
    halo_turn(2, 1, False)
    attend(1, 2, heads)
    sum_z = q_z[y]
    for k in range(1, ny):
        zy_copy(k).wait_recv()
        sum_z += in_y[k - 1].astype(F32)
    sum_y = zs[z_rows(0), :]
    for i in range(1, nz):
        zs_copy(i).wait_recv()
        sum_y += zr[i - 1]
    updated = old + jnp.concatenate([sum_y, sum_z], axis=1)
    squares = jnp.sum(updated * updated, axis=1, keepdims=True)
    new = (updated * (old_norm / jnp.sqrt(squares + NORM_EPS))).astype(BF16)
    fresh[c, y, z_rows(0), :] = new[:, :ag_lanes]
    fresh_z[c, y, z_rows(0), :] = new[:, ag_lanes:]

    def by_copy(k, arrival):
        here = fresh_z.at[c, lax.rem(y + ny - k, ny) if arrival else y, z_rows(0)]
        return remote(here, here, by_s.at[k - 1], by_r.at[k - 1], y_peer[k - 1])

    def bz_copy(i, arrival):
        here = fresh_z.at[c, :, z_rows(nz - i) if arrival else z_rows(0)]
        return remote(here, here, bz_s.at[i - 1], bz_r.at[i - 1], z_peer[i - 1])

    def bd_copy(i, arrival):
        here = fresh_z.at[1 - c if arrival else c, :, z_rows(nz - i)]
        return remote(here, here, bd_s.at[i], bd_r.at[i], mate)

    def az_copy(i, arrival):
        here = fresh.at[c, y, z_rows(nz - i) if arrival else z_rows(0)]
        return remote(here, here, az_s.at[i - 1], az_r.at[i - 1], z_peer[i - 1])

    for i in range(1, nz):
        az_copy(i, False).start()
    for k in range(1, ny):
        by_copy(k, False).start()
    halo_turn(2, 1, True)
    halo_turn(2, 0)
    attend(2, 0, 3)
    for i in range(1, nz):
        az_copy(i, True).wait_recv()

    def ag_copy(way, part, hop):
        origin = toward(1 - way, hop)
        here = fresh.at[c, origin, rows_of[part]]
        n = ag_slot[way, part, hop]
        return remote(here, here, ag_s.at[n], ag_r.at[n], (y_next, y_prev)[way])

    def ag_arrival(way, part, hop):
        origin = toward(1 - way, hop + 1)
        here = fresh.at[c, origin, rows_of[part]]
        n = ag_slot[way, part, hop]
        return remote(here, here, ag_s.at[n], ag_r.at[n], (y_next, y_prev)[way])

    def ad_copy(n, origin, part, arrival):
        here = fresh.at[1 - c if arrival else c, origin, rows_of[part]]
        return remote(here, here, ad_s.at[n], ad_r.at[n], mate)

    for way, part in even:
        if even[way, part] > 0:
            ag_copy(way, part, 0).start()
    passed = []
    for part in range(2):
        passed.append((y, part))
        ad_copy(len(passed) - 1, y, part, False).start()
    for hop in range(ny // 2):
        for way, part in even:
            if hop >= even[way, part]:
                continue
            ag_arrival(way, part, hop).wait_recv()
            if hop + 1 < even[way, part]:
                ag_copy(way, part, hop + 1).start()
            origin = toward(1 - way, hop + 1)
            passed.append((origin, part))
            ad_copy(len(passed) - 1, origin, part, False).start()
        if hop == ny // 2 - 1:
            for i in range(1, nz):
                bz_copy(i, True).wait_recv()
                bd_copy(i, False).start()
        if hop == 0:
            attend(2, 3, heads)
        if hop == 1:
            for k in range(1, ny):
                by_copy(k, True).wait_recv()
            for i in range(1, nz):
                bz_copy(i, False).start()
            bd_copy(0, False).start()
            halo_turn(3, 1)
        if hop == 2:
            halo_turn(3, 0)
            attend(3, 0, heads)
    halo_wait(HOPS - 1)
    attend(HOPS, 0, heads)
    for h in range(heads):
        cols = slice(h * HEAD_DIM, (h + 1) * HEAD_DIM)
        att_v[:, cols] = (acc_s[h] / l_s[h]).astype(BF16)
    for i in range(nz):
        bd_copy(i, True).wait_recv()
    for n, (origin, part) in enumerate(passed):
        ad_copy(n, origin, part, True).wait_recv()

    loads[9].wait()
    queries_y, queries_z = fq[:, :ag_lanes], fq[:, ag_lanes:]

    def weights(ref, which):
        return jnp.concatenate(
            [ref[b % 2, b // 2] for b in range(which * nb, (which + 1) * nb)], axis=0
        )

    def project(which):
        return contract_cols(queries_y, weights(fresh, which)) + contract_cols(
            queries_z, weights(fresh_z, which)
        )

    hidden = (jax.nn.silu(project(0)) * project(1)).astype(BF16)
    out_v[:, :ag_lanes] = jnp.dot(hidden, weights(fresh, 2), preferred_element_type=F32).astype(BF16)
    out_v[:, ag_lanes:] = jnp.dot(hidden, weights(fresh_z, 2), preferred_element_type=F32).astype(BF16)

    for step in range(HOPS):
        halo_send_wait(step)

    @pl.when(straight)
    def _():
        for part in range(2):
            straight_copy(part).wait_send()

    for part in range(2):
        pair_copy(part).wait_send()
    term_copy.wait_send()
    for way, part, hop in slot:
        rs_copy(way, part, hop).wait_send()
    for way, part, hop in ag_slot:
        ag_copy(way, part, hop).wait_send()
    for i in range(1, nz):
        zs_copy(i).wait_send()
        az_copy(i, False).wait_send()
        zz_copy(i).wait_send()
        bz_copy(i, False).wait_send()
    for k in range(1, ny):
        zy_copy(k).wait_send()
        by_copy(k, False).wait_send()
    for i in range(nz):
        bd_copy(i, False).wait_send()
    for n, (origin, part) in enumerate(passed):
        ad_copy(n, origin, part, False).wait_send()


def solution(mesh):
    nz = 4 if mesh.shape["seq"] == 64 else 2
    ny = mesh.shape["seq"] // (2 * nz)

    def body(att_q, att_k, att_v, fast_q, fast_k, fast_v, rates, w_gate, w_up, w_down):
        tok, feat = att_q.shape
        hid = w_gate.shape[1]
        heads = feat // HEAD_DIM
        n_slot = 2 * (ny - 1)
        rs_lanes, ag_lanes = feat - RS_Z, feat - AG_Z
        zrow = BLK // nz
        dma = pltpu.SemaphoreType.DMA
        vmem = pltpu.VMEM
        hbm = pl.BlockSpec(memory_space=pl.ANY)
        return pl.pallas_call(
            functools.partial(kernel, ny, nz, rs_lanes, ag_lanes),
            out_shape=(
                pltpu.VMEM((tok, feat), BF16),
                pltpu.VMEM((tok, feat), BF16),
            ),
            in_specs=[hbm] * 10,
            out_specs=(pl.BlockSpec(memory_space=vmem),) * 2,
            scratch_shapes=[
                vmem((tok, feat), BF16),
                vmem((2, tok, feat), BF16),
                vmem((HOPS, 2, tok, feat), BF16),
                vmem((tok, feat), BF16),
                vmem((2, 2, tok, feat), BF16),
                vmem((1, tok), F32),
                vmem((3, feat, hid), BF16),
                vmem((2, tok, ny * BLK), BF16),
                vmem((tok, ny * BLK), BF16),
                vmem((ny, BLK, rs_lanes), F32),
                vmem((n_slot, BLK // 2, rs_lanes), F32),
                vmem((BLK, rs_lanes), F32),
                vmem((nz - 1, zrow, rs_lanes), F32),
                vmem((BLK, feat), F32),
                vmem((2, ny, BLK, ag_lanes), BF16),
                vmem((ny, BLK, RS_Z), F32),
                vmem((ny, BLK, RS_Z), BF16),
                vmem((nz - 1, ny, zrow, RS_Z), BF16),
                vmem((ny, zrow, RS_Z), F32),
                vmem((ny, zrow, RS_Z), BF16),
                vmem((ny - 1, zrow, RS_Z), BF16),
                vmem((2, ny, BLK, AG_Z), BF16),
                vmem((heads, tok, 1), F32),
                vmem((heads, tok, 1), F32),
                vmem((heads, tok, HEAD_DIM), F32),
                dma((10,)),
                dma((HOPS + 1, 2)),
                dma((HOPS, 2)),
                dma((2,)),
                dma((2,)),
                dma,
                dma,
                dma((n_slot,)),
                dma((n_slot,)),
                dma((nz - 1,)),
                dma((nz - 1,)),
                dma((nz - 1,)),
                dma((nz - 1,)),
                dma((n_slot,)),
                dma((n_slot,)),
                dma((2 * ny,)),
                dma((2 * ny,)),
                dma((nz - 1,)),
                dma((nz - 1,)),
                dma((ny - 1,)),
                dma((ny - 1,)),
                dma((ny - 1,)),
                dma((ny - 1,)),
                dma((nz - 1,)),
                dma((nz - 1,)),
                dma((nz,)),
                dma((nz,)),
            ],
            compiler_params=pltpu.CompilerParams(
                collective_id=0, has_side_effects=True, vmem_limit_bytes=60 * 1024 * 1024
            ),
        )(
            att_q, att_k, att_v, fast_q, fast_k, fast_v, rates.reshape(1, -1),
            w_gate, w_up, w_down,
        )

    rows = P("seq", "head")
    weights = P(None, "head")
    return jax.shard_map(
        body,
        mesh=mesh,
        in_specs=(rows,) * 6 + (P("seq"),) + (weights,) * 3,
        out_specs=(rows, rows),
        check_vma=False,
    )
```

```python
import functools

import jax
import jax.numpy as jnp
from jax import lax
from jax.experimental import pallas as pl
from jax.experimental.pallas import tpu as pltpu
from jax.sharding import PartitionSpec as P

HEAD_DIM = 128
BLK = 128
HOPS = 4
RS_Z = 256
AG_Z = 128
NORM_EPS = 1e-06
LOG2_E = 1.4426950408889634
MASKED = -1e30
MESH = pl.DeviceIdType.MESH
F32 = jnp.float32
BF16 = jnp.bfloat16


def silu_parts(pre_act):
    sig = jax.nn.sigmoid(pre_act)
    return pre_act * sig, sig * (1.0 + pre_act * (1.0 - sig))


def contract_rows(lhs, rhs):
    return lax.dot_general(lhs, rhs, (((0,), (0,)), ((), ())), preferred_element_type=F32)


def contract_cols(lhs, rhs):
    return lax.dot_general(lhs, rhs, (((1,), (1,)), ((), ())), preferred_element_type=F32)


def kernel(
    ny, nz, rs_lanes, ag_lanes,
    aq_h, ak_h, av_h, fq_h, fk_h, fv_h, lr_h, wg_h, wu_h, wd_h,
    att_v, out_v,
    aq, okv, halo, fq, kvf, lr, w3, tt, rt, grad, ry, zs, zr, old_t, fresh,
    g_z, gb_z, in_z, q_z, qb_z, in_y, fresh_z,
    m_s, l_s, acc_s,
    loc, hs, hr, ps, pr, ts, tr, rs_s, rs_r, zs_s, zs_r, az_s, az_r, ag_s, ag_r, ad_s, ad_r,
    zz_s, zz_r, zy_s, zy_r, by_s, by_r, bz_s, bz_r, bd_s, bd_r,
):
    tok, feat = aq.shape
    nb = w3.shape[2] // BLK
    heads = feat // HEAD_DIM
    half = BLK // 2
    zrow = BLK // nz
    s = lax.axis_index("seq")
    total = 2 * ny * nz
    c = lax.rem(s, 2)
    y = lax.rem(s // 2, ny)
    z = s // (2 * ny)
    mate = s + 1 - 2 * c
    y_next = z * 2 * ny + lax.rem(y + 1, ny) * 2 + c
    y_prev = z * 2 * ny + lax.rem(y + ny - 1, ny) * 2 + c
    y_peer = [z * 2 * ny + lax.rem(y + k, ny) * 2 + c for k in range(1, ny)]
    z_peer = [lax.rem(z + i, nz) * 2 * ny + y * 2 + c for i in range(1, nz)]
    chain = {(1, 0): ny // 2, (1, 1): ny // 2, (0, 0): ny // 2 - 1, (0, 1): ny // 2 - 1}
    even = chain

    def remote(src, dst, ssem, rsem, dev):
        return pltpu.make_async_remote_copy(
            src_ref=src, dst_ref=dst, send_sem=ssem, recv_sem=rsem,
            device_id={"seq": dev}, device_id_type=MESH,
        )

    loads = [
        (fk_h, kvf.at[0, 0]), (wg_h, w3.at[0]), (wu_h, w3.at[1]), (lr_h, lr),
        (fv_h, kvf.at[0, 1]), (wd_h, w3.at[2]),
        (aq_h, aq), (ak_h, okv.at[0]), (av_h, okv.at[1]), (fq_h, fq),
    ]
    loads = [pltpu.make_async_copy(src, dst, loc.at[i]) for i, (src, dst) in enumerate(loads)]
    for one in loads:
        one.start()

    barrier = pltpu.get_barrier_semaphore()
    for peer in [mate] + y_peer + z_peer:
        pl.semaphore_signal(barrier, inc=1, device_id={"seq": peer}, device_id_type=MESH)

    @pl.when((c == 1) & (s < total - 1))
    def _():
        pl.semaphore_signal(barrier, inc=1, device_id={"seq": s + 1}, device_id_type=MESH)

    @pl.when((c == 0) & (s > 0))
    def _():
        pl.semaphore_signal(barrier, inc=1, device_id={"seq": s - 1}, device_id_type=MESH)

    @pl.when((c == 0) & (y == 0) & (z > 0))
    def _():
        pl.semaphore_signal(barrier, inc=1, device_id={"seq": s - 2}, device_id_type=MESH)

    beside = (1 - c) * (y // (ny - 1)) * (1 - z // (nz - 1)) + c * (1 - s // (total - 1)) + (1 - c) * ((s + total - 1) // total)

    place = 2 * y + c
    edge = place == 2 * ny - 1
    straight = (place == 2 * ny - 2) & (z < nz - 1)

    def straight_copy(part):
        return remote((ak_h, av_h)[part], halo.at[1, part], hs.at[HOPS, part], hr.at[1, part], s + 2)

    def halo_copy(step, part, dev):
        if step == 0:
            src = (ak_h, av_h)[part]
        else:
            src = halo.at[step - 1, part]
        return remote(src, halo.at[step, part], hs.at[step, part], hr.at[step, part], dev)

    def sends(step):
        due = (s < total - 1) & (s >= step)
        return due & jnp.logical_not(edge) if step == 1 else due

    def halo_send(step):
        @pl.when(sends(step))
        def _():
            for part in range(2):
                halo_copy(step, part, s + 1).start()

    def halo_send_wait(step):
        @pl.when(sends(step))
        def _():
            for part in range(2):
                halo_copy(step, part, s + 1).wait_send()

    def halo_wait(step):
        @pl.when(s >= step + 1)
        def _():
            for part in range(2):
                halo_copy(step, part, s - 1).wait_recv()

    def pair_copy(part):
        return remote((fk_h, fv_h)[part], kvf.at[1, part], ps.at[part], pr.at[part], mate)

    def halo_turn(step, core, at_edge=None):
        due = c == core
        if at_edge is not None:
            due = edge if at_edge else due & jnp.logical_not(edge)

        @pl.when(due)
        def _():
            halo_wait(step - 1)
            halo_send(step)

    scale = HEAD_DIM ** (-0.5) * LOG2_E

    def attend(delta, lo, hi):
        def one_head(h):
            cols = slice(h * HEAD_DIM, (h + 1) * HEAD_DIM)
            kv = okv if delta == 0 else halo.at[delta - 1]
            key, val = kv[0, :, cols], kv[1, :, cols]
            sc = contract_cols(aq[:, cols], key)
            if delta in (0, HOPS):
                qi = lax.broadcasted_iota(jnp.int32, (tok, tok), 0)
                ki = lax.broadcasted_iota(jnp.int32, (tok, tok), 1)
                keep = (ki <= qi) if delta == 0 else (ki > qi)
                sc = jnp.where(keep, sc, MASKED)
            top = jnp.max(sc, axis=1, keepdims=True)
            if delta == 0:
                p = jnp.exp2((sc - top) * scale)
                m_s[h] = top
                l_s[h] = jnp.sum(p, axis=1, keepdims=True)
                acc_s[h] = jnp.dot(p.astype(BF16), val, preferred_element_type=F32)
            else:
                m_old = m_s[h]
                m_new = jnp.maximum(m_old, top)
                p = jnp.exp2((sc - m_new) * scale)
                alpha = jnp.exp2((m_old - m_new) * scale)
                m_s[h] = m_new
                l_s[h] = l_s[h] * alpha + jnp.sum(p, axis=1, keepdims=True)
                acc_s[h] = acc_s[h] * alpha + jnp.dot(p.astype(BF16), val, preferred_element_type=F32)

        if delta == 0:
            for h in range(lo, hi):
                one_head(h)
        else:
            @pl.when(s >= delta)
            def _():
                for h in range(lo, hi):
                    one_head(h)

    loads[0].wait()
    loads[1].wait()
    loads[2].wait()
    loads[3].wait()
    keys = kvf[0, 0]
    eye = lax.broadcasted_iota(jnp.int32, (tok, tok), 0) == lax.broadcasted_iota(jnp.int32, (tok, tok), 1)
    rate = jnp.sum(jnp.where(eye, jnp.broadcast_to(lr[...], (tok, tok)), 0.0), axis=1, keepdims=True)
    if 2 * ny > 3 * nb:
        for b in range(3 * nb, 2 * ny):
            tt[b % 2, :, (b // 2) * BLK:(b // 2 + 1) * BLK] = jnp.zeros((tok, BLK), BF16)

    def put(b, value):
        tt[b % 2, :, (b // 2) * BLK:(b // 2 + 1) * BLK] = value.astype(BF16)

    pre_gate = jnp.dot(keys, w3[0], preferred_element_type=F32)
    pre_up = jnp.dot(keys, w3[1], preferred_element_type=F32)
    loads[4].wait()
    loads[5].wait()
    back = jnp.dot(kvf[0, 1], w3[2], preferred_element_type=F32)
    for i in range(nb):
        cols = slice(i * BLK, (i + 1) * BLK)
        pg, pu, bk = pre_gate[:, cols], pre_up[:, cols], back[:, cols]
        silu, slope = silu_parts(pg)
        rb = rate * bk
        put(i, rb * pu * slope)
        put(nb + i, rb * silu)
        put(2 * nb + i, rate * silu * pu)
    pl.semaphore_wait(barrier, 1 + len(y_peer) + len(z_peer) + beside)
    for part in range(2):
        pair_copy(part).start()
    term_copy = remote(tt.at[1 - c], rt, ts, tr, mate)
    term_copy.start()
    halo_send(0)

    @pl.when(straight)
    def _():
        for part in range(2):
            straight_copy(part).start()


    split = nb * BLK
    width = ny * BLK
    lanes_y, lanes_z = pl.ds(0, rs_lanes), pl.ds(rs_lanes, feat - rs_lanes)

    def add_grads(terms, side, lanes, into, first):
        low = contract_rows(terms(0, split), kvf[side, 0, :, lanes]).reshape(nb, BLK, -1)
        high = contract_rows(terms(split, width), kvf[side, 1, :, lanes]).reshape(ny - nb, BLK, -1)
        if first:
            into[0:nb], into[nb:ny] = low, high
        else:
            into[0:nb] += low
            into[nb:ny] += high

    def own_terms(lo, hi):
        return tt[c, :, lo:hi]

    def mate_terms(lo, hi):
        return rt[:, lo:hi]

    add_grads(own_terms, 0, lanes_z, g_z, True)
    add_grads(own_terms, 0, lanes_y, grad, True)
    for i in range(6, 9):
        loads[i].wait()
    attend(0, 0, 1)
    term_copy.wait_recv()
    for part in range(2):
        pair_copy(part).wait_recv()
    add_grads(mate_terms, 1, lanes_z, g_z, False)

    def z_rows(i):
        return pl.ds(pl.multiple_of(lax.rem(z + i, nz) * zrow, zrow), zrow)

    gb_z[...] = g_z[...].astype(BF16)

    def zz_copy(i):
        return remote(gb_z.at[:, z_rows(i)], in_z.at[i - 1], zz_s.at[i - 1], zz_r.at[i - 1], z_peer[i - 1])

    def zy_copy(k):
        return remote(
            qb_z.at[lax.rem(y + k, ny)], in_y.at[k - 1], zy_s.at[k - 1], zy_r.at[k - 1], y_peer[k - 1]
        )

    for i in range(1, nz):
        zz_copy(i).start()
    add_grads(mate_terms, 1, lanes_y, grad, False)

    def turn_z():
        got = g_z[:, z_rows(0), :]
        for i in range(1, nz):
            zz_copy(i).wait_recv()
            got += in_z[i - 1].astype(F32)
        q_z[...] = got
        qb_z[...] = got.astype(BF16)
        for k in range(1, ny):
            zy_copy(k).start()

    rows_of = [pl.ds(0, half), pl.ds(half, half)]
    slot, ag_slot = {}, {}
    for way in range(2):
        for part in range(2):
            for hop in range(chain[way, part]):
                slot[way, part, hop] = len(slot)
            for hop in range(even[way, part]):
                ag_slot[way, part, hop] = len(ag_slot)

    def toward(way, dist):
        return lax.rem(y + dist, ny) if way == 0 else lax.rem(y + ny - dist, ny)

    def rs_copy(way, part, hop):
        if hop == 0:
            src = grad.at[toward(way, chain[way, part]), rows_of[part]]
        else:
            src = ry.at[slot[way, part, hop - 1]]
        n = slot[way, part, hop]
        return remote(src, ry.at[n], rs_s.at[n], rs_r.at[n], (y_next, y_prev)[way])

    for way, part in chain:
        rs_copy(way, part, 0).start()
    attend(0, 1, 3)

    def rs_step(way, hop):
        for part in range(2):
            rs_copy(way, part, hop).wait_recv()
            if hop + 1 < chain[way, part]:
                n = slot[way, part, hop]
                ry[n] += grad[toward(way, chain[way, part] - hop - 1), rows_of[part]]
                rs_copy(way, part, hop + 1).start()

    rs_step(1, 0)
    attend(0, 3, heads)
    rs_step(0, 0)
    rs_step(1, 1)
    halo_wait(0)

    @pl.when(c == 0)
    def _():
        halo_send(1)

    rs_step(0, 1)
    attend(1, 0, 2)
    rs_step(1, 2)
    turn_z()

    @pl.when(c == 1)
    def _():
        halo_send(1)

    rs_step(0, 2)
    rs_step(1, 3)
    for part in range(2):
        got = grad[y, rows_of[part]]
        for way in range(2):
            if chain[way, part] > 0:
                got += ry[slot[way, part, chain[way, part] - 1]]
        zs[rows_of[part]] = got

    def zs_copy(i):
        return remote(zs.at[z_rows(i)], zr.at[i - 1], zs_s.at[i - 1], zs_r.at[i - 1], z_peer[i - 1])

    for i in range(1, nz):
        zs_copy(i).start()
    own_b = 2 * y + c
    src_b = jnp.minimum(own_b, 3 * nb - 1)
    old_cols = pl.ds(pl.multiple_of(lax.rem(src_b, nb) * BLK, BLK), BLK)
    old_t[...] = w3[src_b // nb, :, old_cols].astype(F32).T
    old = old_t[z_rows(0), :]
    old_norm = jnp.sqrt(jnp.sum(old * old, axis=1, keepdims=True))
    halo_turn(2, 1, False)
    attend(1, 2, heads)
    sum_z = q_z[y]
    for k in range(1, ny):
        zy_copy(k).wait_recv()
        sum_z += in_y[k - 1].astype(F32)
    sum_y = zs[z_rows(0), :]
    for i in range(1, nz):
        zs_copy(i).wait_recv()
        sum_y += zr[i - 1]
    updated = old + jnp.concatenate([sum_y, sum_z], axis=1)
    squares = jnp.sum(updated * updated, axis=1, keepdims=True)
    new = (updated * (old_norm / jnp.sqrt(squares + NORM_EPS))).astype(BF16)
    fresh[c, y, z_rows(0), :] = new[:, :ag_lanes]
    fresh_z[c, y, z_rows(0), :] = new[:, ag_lanes:]

    def by_copy(k, arrival):
        here = fresh_z.at[c, lax.rem(y + ny - k, ny) if arrival else y, z_rows(0)]
        return remote(here, here, by_s.at[k - 1], by_r.at[k - 1], y_peer[k - 1])

    def bz_copy(i, arrival):
        here = fresh_z.at[c, :, z_rows(nz - i) if arrival else z_rows(0)]
        return remote(here, here, bz_s.at[i - 1], bz_r.at[i - 1], z_peer[i - 1])

    def bd_copy(i, arrival):
        here = fresh_z.at[1 - c if arrival else c, :, z_rows(nz - i)]
        return remote(here, here, bd_s.at[i], bd_r.at[i], mate)

    def az_copy(i, arrival):
        here = fresh.at[c, y, z_rows(nz - i) if arrival else z_rows(0)]
        return remote(here, here, az_s.at[i - 1], az_r.at[i - 1], z_peer[i - 1])

    for i in range(1, nz):
        az_copy(i, False).start()
    for k in range(1, ny):
        by_copy(k, False).start()
    halo_turn(2, 1, True)
    halo_turn(2, 0)
    attend(2, 0, 3)
    for i in range(1, nz):
        az_copy(i, True).wait_recv()

    def ag_copy(way, part, hop):
        origin = toward(1 - way, hop)
        here = fresh.at[c, origin, rows_of[part]]
        n = ag_slot[way, part, hop]
        return remote(here, here, ag_s.at[n], ag_r.at[n], (y_next, y_prev)[way])

    def ag_arrival(way, part, hop):
        origin = toward(1 - way, hop + 1)
        here = fresh.at[c, origin, rows_of[part]]
        n = ag_slot[way, part, hop]
        return remote(here, here, ag_s.at[n], ag_r.at[n], (y_next, y_prev)[way])

    def ad_copy(n, origin, part, arrival):
        here = fresh.at[1 - c if arrival else c, origin, rows_of[part]]
        return remote(here, here, ad_s.at[n], ad_r.at[n], mate)

    for way, part in even:
        if even[way, part] > 0:
            ag_copy(way, part, 0).start()
    passed = []
    for part in range(2):
        passed.append((y, part))
        ad_copy(len(passed) - 1, y, part, False).start()
    for hop in range(ny // 2):
        for way, part in even:
            if hop >= even[way, part]:
                continue
            ag_arrival(way, part, hop).wait_recv()
            if hop + 1 < even[way, part]:
                ag_copy(way, part, hop + 1).start()
            origin = toward(1 - way, hop + 1)
            passed.append((origin, part))
            ad_copy(len(passed) - 1, origin, part, False).start()
        if hop == ny // 2 - 1:
            for i in range(1, nz):
                bz_copy(i, True).wait_recv()
                bd_copy(i, False).start()
        if hop == 0:
            attend(2, 3, heads)
        if hop == 1:
            for k in range(1, ny):
                by_copy(k, True).wait_recv()
            for i in range(1, nz):
                bz_copy(i, False).start()
            bd_copy(0, False).start()
            halo_turn(3, 1)
        if hop == 2:
            halo_turn(3, 0)
            attend(3, 0, heads)
    halo_wait(HOPS - 1)
    attend(HOPS, 0, heads)
    for h in range(heads):
        cols = slice(h * HEAD_DIM, (h + 1) * HEAD_DIM)
        att_v[:, cols] = (acc_s[h] / l_s[h]).astype(BF16)
    for i in range(nz):
        bd_copy(i, True).wait_recv()
    for n, (origin, part) in enumerate(passed):
        ad_copy(n, origin, part, True).wait_recv()

    loads[9].wait()
    queries_y, queries_z = fq[:, :ag_lanes], fq[:, ag_lanes:]

    def weights(ref, which):
        return jnp.concatenate(
            [ref[b % 2, b // 2] for b in range(which * nb, (which + 1) * nb)], axis=0
        )

    def project(which):
        return contract_cols(queries_y, weights(fresh, which)) + contract_cols(
            queries_z, weights(fresh_z, which)
        )

    hidden = (jax.nn.silu(project(0)) * project(1)).astype(BF16)
    out_v[:, :ag_lanes] = jnp.dot(hidden, weights(fresh, 2), preferred_element_type=F32).astype(BF16)
    out_v[:, ag_lanes:] = jnp.dot(hidden, weights(fresh_z, 2), preferred_element_type=F32).astype(BF16)

    for step in range(HOPS):
        halo_send_wait(step)

    @pl.when(straight)
    def _():
        for part in range(2):
            straight_copy(part).wait_send()

    for part in range(2):
        pair_copy(part).wait_send()
    term_copy.wait_send()
    for way, part, hop in slot:
        rs_copy(way, part, hop).wait_send()
    for way, part, hop in ag_slot:
        ag_copy(way, part, hop).wait_send()
    for i in range(1, nz):
        zs_copy(i).wait_send()
        az_copy(i, False).wait_send()
        zz_copy(i).wait_send()
        bz_copy(i, False).wait_send()
    for k in range(1, ny):
        zy_copy(k).wait_send()
        by_copy(k, False).wait_send()
    for i in range(nz):
        bd_copy(i, False).wait_send()
    for n, (origin, part) in enumerate(passed):
        ad_copy(n, origin, part, False).wait_send()


def solution(mesh):
    nz = 4 if mesh.shape["seq"] == 64 else 2
    ny = mesh.shape["seq"] // (2 * nz)

    def body(att_q, att_k, att_v, fast_q, fast_k, fast_v, rates, w_gate, w_up, w_down):
        tok, feat = att_q.shape
        hid = w_gate.shape[1]
        heads = feat // HEAD_DIM
        n_slot = 2 * (ny - 1)
        rs_lanes, ag_lanes = feat - RS_Z, feat - AG_Z
        zrow = BLK // nz
        dma = pltpu.SemaphoreType.DMA
        vmem = pltpu.VMEM
        hbm = pl.BlockSpec(memory_space=pl.ANY)
        return pl.pallas_call(
            functools.partial(kernel, ny, nz, rs_lanes, ag_lanes),
            out_shape=(
                pltpu.VMEM((tok, feat), BF16),
                pltpu.VMEM((tok, feat), BF16),
            ),
            in_specs=[hbm] * 10,
            out_specs=(pl.BlockSpec(memory_space=vmem),) * 2,
            scratch_shapes=[
                vmem((tok, feat), BF16),
                vmem((2, tok, feat), BF16),
                vmem((HOPS, 2, tok, feat), BF16),
                vmem((tok, feat), BF16),
                vmem((2, 2, tok, feat), BF16),
                vmem((1, tok), F32),
                vmem((3, feat, hid), BF16),
                vmem((2, tok, ny * BLK), BF16),
                vmem((tok, ny * BLK), BF16),
                vmem((ny, BLK, rs_lanes), F32),
                vmem((n_slot, BLK // 2, rs_lanes), F32),
                vmem((BLK, rs_lanes), F32),
                vmem((nz - 1, zrow, rs_lanes), F32),
                vmem((BLK, feat), F32),
                vmem((2, ny, BLK, ag_lanes), BF16),
                vmem((ny, BLK, RS_Z), F32),
                vmem((ny, BLK, RS_Z), BF16),
                vmem((nz - 1, ny, zrow, RS_Z), BF16),
                vmem((ny, zrow, RS_Z), F32),
                vmem((ny, zrow, RS_Z), BF16),
                vmem((ny - 1, zrow, RS_Z), BF16),
                vmem((2, ny, BLK, AG_Z), BF16),
                vmem((heads, tok, 1), F32),
                vmem((heads, tok, 1), F32),
                vmem((heads, tok, HEAD_DIM), F32),
                dma((10,)),
                dma((HOPS + 1, 2)),
                dma((HOPS, 2)),
                dma((2,)),
                dma((2,)),
                dma,
                dma,
                dma((n_slot,)),
                dma((n_slot,)),
                dma((nz - 1,)),
                dma((nz - 1,)),
                dma((nz - 1,)),
                dma((nz - 1,)),
                dma((n_slot,)),
                dma((n_slot,)),
                dma((2 * ny,)),
                dma((2 * ny,)),
                dma((nz - 1,)),
                dma((nz - 1,)),
                dma((ny - 1,)),
                dma((ny - 1,)),
                dma((ny - 1,)),
                dma((ny - 1,)),
                dma((nz - 1,)),
                dma((nz - 1,)),
                dma((nz,)),
                dma((nz,)),
            ],
            compiler_params=pltpu.CompilerParams(
                collective_id=0, has_side_effects=True, vmem_limit_bytes=60 * 1024 * 1024
            ),
        )(
            att_q, att_k, att_v, fast_q, fast_k, fast_v, rates.reshape(1, -1),
            w_gate, w_up, w_down,
        )

    rows = P("seq", "head")
    weights = P(None, "head")
    return jax.shard_map(
        body,
        mesh=mesh,
        in_specs=(rows,) * 6 + (P("seq"),) + (weights,) * 3,
        out_specs=(rows, rows),
        check_vma=False,
    )
```
